256 devices in a mesh: gx: 8 (over z_lo, x), gy: 4 (over z_hi), gz: 8 (over y, core).
Axes of the slice: x: 4, y: 4, z: 8 (z_hi: 4, z_lo: 2; z = z_hi * 2 + z_lo), core: 2. Of those that a mesh axis runs over, the one named last changes fastest.
Arguments:
- displacement: bfloat16 [3, 32, 128, 128], P(None, 'gx', 'gy', 'gz'), may hold values from -6 to 6
- lift_weight: bfloat16 [27, 64, 3], replicated, may hold values from -1 to 1
- encode_weight: bfloat16 [27, 64, 64], replicated, may hold values from -0.21875 to 0.21875
- downward_weight: bfloat16 [8, 128, 64], replicated, may hold values from -0.375 to 0.375
- middle_first: bfloat16 [27, 128, 128], replicated, may hold values from -0.15625 to 0.15625
- middle_second: bfloat16 [27, 128, 128], replicated, may hold values from -0.15625 to 0.15625
- up_weight: bfloat16 [8, 64, 128], replicated, may hold values from -0.75 to 0.75
- decode_weight: bfloat16 [27, 64, 128], replicated, may hold values from -0.15625 to 0.15625
- head_weight: bfloat16 [3, 64], replicated, may hold values from -1 to 1
Outputs:
- imitated: float32 [3, 32, 128, 128], P(None, 'gx', 'gy', 'gz')
The draws below stay inside these ranges and needn't reach their ends.
All inputs are finite; a program needn't handle non-finite values.
Results may differ from the reference program's by a relative error of at most 0.0055.
Values may be sent and summed in bfloat16 or wider, within the bound.
A program may use at most 64 MiB of HBM per device.

```python
import jax
import jax.numpy as jnp

C1 = 64
C2 = 128
NX = 32
NY = 128
NZ = 128


def levels(stream_key, shape, pieces, low, top_value):
    loudness, own = 1.0, jax.random.fold_in(stream_key, 6)
    for position, parts in pieces:
        steps = jnp.exp(jax.random.uniform(jax.random.fold_in(own, position), (parts,), jnp.float32, low / len(pieces), top_value / len(pieces)))
        loudness = loudness * jnp.repeat(steps, shape[position] // parts).reshape([-1 if axis == position else 1 for axis in range(len(shape))])
    return loudness


def noise(stream_key, shape, scale, bound, shards=(), kind=jnp.bfloat16):
    entries = jax.random.normal(stream_key, shape, jnp.float32) * scale
    if len(shards) > 0:
        entries = levels(stream_key, shape, shards, -0.22, 0.18) * entries
    return jnp.clip(entries, min=-bound, max=bound).astype(kind)


def setup_inputs(seed: int = 0) -> dict:
    streams_of = jax.random.split(jax.random.key(seed), 10)
    return {
        "displacement": noise(streams_of[0], (3, NX, NY, NZ), 1.0, 6.0, ((1, 8), (2, 4), (3, 8))),
        "lift_weight": noise(streams_of[1], (27, C1, 3), (81 // 2) ** -0.5, 1.0),
        "encode_weight": noise(streams_of[2], (27, C1, C1), (27 * C1 // 2) ** -0.5, 0.21875),
        "downward_weight": noise(streams_of[3], (8, C2, C1), (4 * C1) ** -0.5, 0.375),
        "middle_first": noise(streams_of[4], (27, C2, C2), (27 * C2 // 2) ** -0.5, 0.15625),
        "middle_second": noise(streams_of[5], (27, C2, C2), (27 * C2 // 2) ** -0.5, 0.15625),
        "up_weight": noise(streams_of[6], (8, C1, C2), (C2 // 2) ** -0.5, 0.75),
        "decode_weight": noise(streams_of[7], (27, C1, 2 * C1), (27 * C1) ** -0.5, 0.15625),
        "head_weight": noise(streams_of[8], (3, C1), (C1 // 2) ** -0.5, 1.0),
    }


def apply_relu(value):
    return jnp.where(value > 0, value, 0.1 * value)


def conv_periodic(field, weight_tensor):
    padded = jnp.pad(field, ((0, 0), (1, 1), (1, 1), (1, 1)), mode="wrap")
    size_x, size_y, size_z = field.shape[1], field.shape[2], field.shape[3]
    weights32 = weight_tensor.astype(jnp.float32)
    summed = jnp.zeros((weight_tensor.shape[1], size_x, size_y, size_z), jnp.float32)
    for offset in range(27):
        a, b, c = offset // 9, (offset // 3) % 3, offset % 3
        window = padded[:, a:a + size_x, b:b + size_y, c:c + size_z].astype(jnp.float32)
        summed = summed + jnp.einsum("oi,ixyz->oxyz", weights32[offset], window)
    return summed


def reduce_resolution(fine_level, weight_tensor):
    chans, size_x, size_y, size_z = fine_level.shape
    blocks = fine_level.reshape(chans, size_x // 2, 2, size_y // 2, 2, size_z // 2, 2).astype(jnp.float32)
    kernel = weight_tensor.reshape(2, 2, 2, weight_tensor.shape[1], weight_tensor.shape[2]).astype(jnp.float32)
    return jnp.einsum("abcoi,ixaybzc->oxyz", kernel, blocks)


def upsample(coarse_field, weight_tensor):
    chans, size_x, size_y, size_z = coarse_field.shape
    kernel = weight_tensor.reshape(2, 2, 2, weight_tensor.shape[1], weight_tensor.shape[2]).astype(jnp.float32)
    result = jnp.einsum("abcoi,ixyz->oxaybzc", kernel, coarse_field.astype(jnp.float32))
    return result.reshape(weight_tensor.shape[1], 2 * size_x, 2 * size_y, 2 * size_z)


def reference(displacement, lift_weight, encode_weight, downward_weight, middle_first, middle_second, up_weight, decode_weight, head_weight):
    first = apply_relu(conv_periodic(displacement, lift_weight)).astype(jnp.bfloat16)
    skip_link = apply_relu(conv_periodic(first, encode_weight)).astype(jnp.bfloat16)
    coarse_level = apply_relu(reduce_resolution(skip_link, downward_weight)).astype(jnp.bfloat16)
    middle = apply_relu(conv_periodic(coarse_level, middle_first)).astype(jnp.bfloat16)
    deep = apply_relu(conv_periodic(middle, middle_second)).astype(jnp.bfloat16)
    upsampled = apply_relu(upsample(deep, up_weight)).astype(jnp.bfloat16)
    stacked = jnp.concatenate([skip_link, upsampled], axis=0)
    joined = apply_relu(conv_periodic(stacked, decode_weight)).astype(jnp.bfloat16)
    head = jnp.einsum("oi,ixyz->oxyz", head_weight.astype(jnp.float32), joined.astype(jnp.float32))
    return displacement.astype(jnp.float32) + head
```

```python
import jax
import jax.numpy as jnp
import numpy as np
from jax import lax
from jax.experimental import pallas as pl
from jax.experimental.pallas import tpu as pltpu
from jax.sharding import PartitionSpec as P

BF = jnp.bfloat16
F32 = jnp.float32


def act(v):
    return jnp.where(v > 0, v, 0.1 * v)


def lift_selection():
    sel = np.zeros((3, 4, 192, 27), np.float32)
    for oy in range(2):
        for oz in range(2):
            for dx in range(3):
                for dy in range(2):
                    for dz in range(2):
                        for jy in range(2):
                            for jz in range(2):
                                b, c = 2 * dy + jy - oy, 2 * dz + jz - oz
                                if 0 <= b < 3 and 0 <= c < 3:
                                    for ch in range(3):
                                        row = (((dx * 2 + dy) * 2 + dz) * 16 + (jy * 2 + jz) * 3 + ch)
                                        sel[ch, oy * 2 + oz, row, 9 * dx + 3 * b + c] = 1
    return sel.reshape(3, 768, 27)


def dot(a, b):
    return jnp.dot(a, b, preferred_element_type=F32)


def unet(
    qt, lw, sel, ew, dw, m1, m2, uw, cw, hw,
    out,
    patch, wl, we, wd, wm1, wm2, wu, wc, wh,
    f0, f1, skip, coarse, middle, deep, ks, ku, joined,
):
    w = dot(sel[0], lw[0]) + dot(sel[1], lw[1]) + dot(sel[2], lw[2])
    w = w.reshape(4, 192, 64)
    wl[:, 0:128] = jnp.concatenate([w[0], w[1]], axis=1).astype(BF)
    wl[:, 128:256] = jnp.concatenate([w[2], w[3]], axis=1).astype(BF)

    def pair_tiles(src, a, b):
        taps = [src[9 * a + 3 * b + c].astype(F32) for c in range(3)]
        none = jnp.zeros_like(taps[0])
        for m in range(4):
            lo = taps[m] if m < 3 else none
            hi = taps[m - 1] if m > 0 else none
            yield m, jnp.transpose(jnp.concatenate([lo, hi], axis=0)).astype(BF)

    we[...] = jnp.zeros_like(we)
    wc[...] = jnp.zeros_like(wc)
    wm1[...] = jnp.zeros_like(wm1)
    wm2[...] = jnp.zeros_like(wm2)
    for a in range(3):
        for b in range(3):
            for m, tile in pair_tiles(ew, a, b):
                dz, jz = m // 2, m % 2
                for dy in range(2):
                    for jy in range(2):
                        oy = 2 * dy + jy - b
                        if 0 <= oy < 2:
                            row = ((a * 2 + dy) * 2 + dz) * 256 + (jy * 2 + jz) * 64
                            we[row : row + 64, oy * 128 : oy * 128 + 128] = tile
            for m, tile in pair_tiles(cw, a, b):
                dz, jz = m // 2, m % 2
                for dy in range(2):
                    for jy in range(2):
                        oy = 2 * dy + jy - b
                        if 0 <= oy < 2:
                            for s in range(2):
                                row = (((s * 3 + a) * 2 + dy) * 2 + dz) * 256 + (jy * 2 + jz) * 64
                                wc[row : row + 64, oy * 128 : oy * 128 + 128] = tile[s * 64 : s * 64 + 64]
            for c in range(3):
                for src, dst in ((m1, wm1), (m2, wm2)):
                    tile = jnp.transpose(src[9 * a + 3 * b + c].astype(F32)).astype(BF)
                    for dy in range(2):
                        for jy in range(2):
                            oy = 2 * dy + jy - b
                            if 0 <= oy < 2:
                                row = ((a * 2 + dy) * 3 + c) * 256 + jy * 128
                                dst[row : row + 128, oy * 128 : oy * 128 + 128] = tile
    wd[...] = dw[...].reshape(2, 256, 128)
    for a in range(2):
        for b in range(2):
            pairs = jnp.concatenate([uw[4 * a + 2 * b + 1], uw[4 * a + 2 * b]], axis=0).astype(F32)
            wu[a, :, b * 128 : b * 128 + 128] = jnp.transpose(pairs).astype(BF)
    wh[...] = jnp.zeros_like(wh)
    for g in range(4):
        wh[3 * g : 3 * g + 3, 64 * g : 64 * g + 64] = hw[...].astype(F32)

    @pl.loop(0, 20)
    def _(x):
        q = qt[x].astype(F32)
        for dy in range(2):
            for dz in range(2):
                s = dy * 16 + dz
                r = pltpu.roll(q, 384 - s, axis=1) if s else q
                g = dy * 2 + dz
                patch[x, 16 * g : 16 * g + 16, :] = r.astype(BF)

    @pl.loop(0, 18)
    def _(x):
        p = patch[pl.ds(x, 3)].reshape(192, 384)
        v = lax.dot_general(p, wl[...], (((0,), (0,)), ((), ())), preferred_element_type=F32)
        v = act(v)
        f0[x] = v.astype(BF)
        f1[x] = pltpu.roll(v, 383, axis=0).astype(BF)

    @pl.loop(0, 8)
    def _(i):
        for h in range(2):
            x = 2 * i + h
            taps = []
            for a in range(3):
                for dy in range(2):
                    for src in (f0, f1):
                        taps.append(src[x + a, dy * 16 : dy * 16 + 352, :])
            v = dot(jnp.concatenate(taps, axis=1), we[...])
            skip[x] = act(v).astype(BF)

    @pl.loop(0, 8)
    def _(x):
        lhs = jnp.concatenate([skip[2 * x], skip[2 * x + 1]], axis=1)
        v = act(dot(lhs, wd[...].reshape(512, 128)))
        for c in range(3):
            r = pltpu.roll(v, 352 - c, axis=0) if c else v
            r = r.reshape(11, 2, 16, 128)
            coarse[c, x, :, 0:128] = r[:, 0].reshape(176, 128).astype(BF)
            coarse[c, x, :, 128:256] = r[:, 1].reshape(176, 128).astype(BF)

    @pl.loop(0, 3)
    def _(i):
        for h in range(2):
            x = 2 * i + h
            taps = []
            for a in range(3):
                for dy in range(2):
                    for c in range(3):
                        taps.append(coarse[c, x + a, dy * 16 : dy * 16 + 160, :])
            v = act(dot(jnp.concatenate(taps, axis=1), wm1[...]))
            for c in range(3):
                r = pltpu.roll(v, 160 - c, axis=0) if c else v
                middle[c, x] = r.astype(BF)

    @pl.loop(0, 2)
    def _(i):
        for h in range(2):
            x = 2 * i + h
            taps = []
            for a in range(3):
                for dy in range(2):
                    for c in range(3):
                        taps.append(middle[c, x + a, dy * 16 : dy * 16 + 144, :])
            v = act(dot(jnp.concatenate(taps, axis=1), wm2[...]))
            deep[x] = v.astype(BF)

    low = lax.broadcasted_iota(jnp.int32, (17, 16, 128), 2) < 64

    def spread(dst, f, blocks):
        for dz in range(2):
            r = pltpu.roll(blocks, 15, axis=1) if dz else blocks
            r = r[:, 0:8]
            for dy in range(2):
                dst[dy, dz, f] = r[dy : dy + 16].reshape(128, 256).astype(BF)

    @pl.loop(0, 6)
    def _(f):
        v = skip[f + 5].astype(F32).reshape(22, 16, 256)
        halves = []
        for jy in range(2):
            s = v[2 + jy : 19 + jy, :, 128 - 128 * jy : 256 - 128 * jy]
            t = jnp.where(low, pltpu.roll(s, 13, axis=1), pltpu.roll(s, 14, axis=1))
            halves.append(pltpu.roll(t, 64, axis=2))
        spread(ks, f, jnp.concatenate(halves, axis=2))

    @pl.loop(0, 6)
    def _(f):
        xd = (f + 1) // 2
        a = (f + 1) % 2
        d = deep[xd]
        us = []
        for jy in range(2):
            us.append(act(dot(d[:, jy * 128 : jy * 128 + 128], wu[a])).reshape(9, 1, 16, 256))
        u = jnp.concatenate(us, axis=1).reshape(18, 16, 256)
        halves = []
        for jy in range(2):
            s = u[jy : 17 + jy, :, 128 - 128 * jy : 256 - 128 * jy]
            halves.append(jnp.where(low, s, pltpu.roll(s, 15, axis=1)))
        spread(ku, f, jnp.concatenate(halves, axis=2))

    @pl.loop(0, 2)
    def _(i):
        x = 2 * i
        taps = []
        for src in (ks, ku):
            for a in range(3):
                for dy in range(2):
                    for dz in range(2):
                        taps.append(src[dy, dz, pl.ds(x + a, 2)].reshape(256, 256))
        v = act(dot(jnp.concatenate(taps, axis=1), wc[...])).astype(BF)
        for h in range(2):
            j = v[h * 128 : h * 128 + 128]
            out[x + h] = lax.dot_general(
                wh[...].astype(BF), j, (((1,), (1,)), ((), ())), preferred_element_type=F32
            )


def network(qt, lw, ew, dw, m1, m2, uw, cw, hw):
    sel = jnp.asarray(lift_selection(), BF)
    vm = pl.BlockSpec(memory_space=pltpu.VMEM)
    return pl.pallas_call(
        unet,
        out_shape=jax.ShapeDtypeStruct((4, 16, 128), F32),
        in_specs=[vm] * 10,
        out_specs=vm,
        scratch_shapes=[
            pltpu.VMEM((20, 64, 384), BF),
            pltpu.VMEM((192, 256), BF),
            pltpu.VMEM((3072, 256), BF),
            pltpu.VMEM((2, 256, 128), BF),
            pltpu.VMEM((4608, 256), BF),
            pltpu.VMEM((4608, 256), BF),
            pltpu.VMEM((2, 128, 256), BF),
            pltpu.VMEM((6144, 256), BF),
            pltpu.VMEM((16, 256), F32),
            pltpu.VMEM((18, 384, 256), BF),
            pltpu.VMEM((18, 384, 256), BF),
            pltpu.VMEM((16, 352, 256), BF),
            pltpu.VMEM((3, 8, 176, 256), BF),
            pltpu.VMEM((3, 6, 160, 256), BF),
            pltpu.VMEM((4, 144, 256), BF),
            pltpu.VMEM((2, 2, 6, 128, 256), BF),
            pltpu.VMEM((2, 2, 6, 128, 256), BF),
            pltpu.VMEM((8, 128), F32),
        ],
        compiler_params=pltpu.CompilerParams(vmem_limit_bytes=56 * 1024 * 1024),
    )(qt, jnp.transpose(lw, (2, 0, 1)), sel, ew, jnp.transpose(dw, (0, 2, 1)), m1, m2, uw, cw, hw)


def ring(value, axis, step):
    n = lax.axis_size(axis)
    return lax.ppermute(value, axis, [(i, (i + step) % n) for i in range(n)])


def local(d, lw, ew, dw, m1, m2, uw, cw, hw):
    wide = jnp.concatenate(
        [ring(d, "gx", 2), ring(d, "gx", 1), d, ring(d, "gx", -1), ring(d, "gx", -2)], axis=1
    )
    for axis, dim in (("gy", 2), ("gz", 3)):
        size = wide.shape[dim]
        head = lax.slice_in_dim(wide, 0, 8, axis=dim)
        tail = lax.slice_in_dim(wide, size - 8, size, axis=dim)
        wide = jnp.concatenate([ring(tail, axis, 1), wide, ring(head, axis, -1)], axis=dim)
    qt = wide.reshape(3, 20, 24, 2, 16, 2).transpose(1, 3, 5, 0, 2, 4).reshape(20, 12, 384)
    qt = jnp.pad(qt, ((0, 0), (0, 4), (0, 0)))
    head = network(qt, lw, ew, dw, m1, m2, uw, cw, hw)
    head = head[:, :12].reshape(4, 2, 2, 3, 16, 8).transpose(3, 0, 4, 1, 5, 2).reshape(3, 4, 32, 16)
    return d.astype(F32) + head


def solution(mesh):
    placed = (P(None, "gx", "gy", "gz"), P(), P(), P(), P(), P(), P(), P(), P())
    return jax.shard_map(
        local, mesh=mesh, in_specs=placed, out_specs=P(None, "gx", "gy", "gz"), check_vma=False
    )
```

```python
import jax
import jax.numpy as jnp
import numpy as np
from jax import lax
from jax.experimental import pallas as pl
from jax.experimental.pallas import tpu as pltpu
from jax.sharding import PartitionSpec as P

BF = jnp.bfloat16
F32 = jnp.float32


def act(v):
    return jnp.where(v > 0, v, 0.1 * v)


def lift_selection():
    sel = np.zeros((3, 4, 192, 27), np.float32)
    for oy in range(2):
        for oz in range(2):
            for dx in range(3):
                for dy in range(2):
                    for dz in range(2):
                        for jy in range(2):
                            for jz in range(2):
                                b, c = 2 * dy + jy - oy, 2 * dz + jz - oz
                                if 0 <= b < 3 and 0 <= c < 3:
                                    for ch in range(3):
                                        row = (((dx * 2 + dy) * 2 + dz) * 16 + (jy * 2 + jz) * 3 + ch)
                                        sel[ch, oy * 2 + oz, row, 9 * dx + 3 * b + c] = 1
    return sel.reshape(3, 768, 27)


def place_columns():
    place = np.zeros((32, 256), np.float32)
    for jy in range(2):
        for lane in range(128):
            place[2 * (lane // 8) + jy, 128 * jy + lane] = 1
    return place


def gather_rows():
    rows = np.zeros((2, 64, 192), np.float32)
    for jy in range(2):
        for x in range(4):
            for z in range(16):
                for c in range(3):
                    rows[jy, 16 * x + jy * 6 + (z % 2) * 3 + c, 64 * c + 16 * x + z] = 1
    return rows


def widen_lanes():
    wide = np.zeros((384, 256), np.float32)
    slab = np.zeros((384, 256), np.float32)
    for piece, (first, shift) in enumerate(((0, 4), (4, -4), (0, 12))):
        for z in range(first, 8 if piece < 2 else 4):
            for y in range(16):
                wide[128 * piece + 8 * y + z, 16 * y + z + shift] = 1
            for i in range(4):
                for y in range(4):
                    slab[128 * piece + 32 * i + 8 * y + z, 64 * i + 16 * y + z + shift] = 1
    return wide, slab


def dot(a, b):
    return jnp.dot(a, b, preferred_element_type=F32)


def remote(src, dst, send, recv, **where):
    return pltpu.make_async_remote_copy(
        src_ref=src, dst_ref=dst, send_sem=send, recv_sem=recv,
        device_id=where, device_id_type=pl.DeviceIdType.MESH,
    )


def unet(
    disp, place, rows, lw_hbm, sel_hbm, wide_hbm, slab_hbm,
    ew_hbm, dw_hbm, m1_hbm, m2_hbm, uw_hbm, cw_hbm, hw,
    out,
    layers, left, right, slab_out, slab_in, sides, slabs, heads, qt,
    lw, sel, wide, slab, ew, dw, m1, m2, uw, cw,
    patch, wl, we, wd, wm1, wm2, wu, wc, wh,
    f0, f1, skip, coarse, middle, deep, ks, ku,
    load_sem, x_send, x_recv, n_send, n_recv,
):
    gx, gy, gz = lax.axis_index("gx"), lax.axis_index("gy"), lax.axis_index("gz")
    nx, ny, nz = lax.axis_size("gx"), lax.axis_size("gy"), lax.axis_size("gz")

    def at_x(step):
        return lax.rem(gx + nx + step, nx)

    def at_yz(sy, sz):
        return {"gy": lax.rem(gy + ny + sy, ny), "gz": lax.rem(gz + nz + sz, nz)}

    around = [(sy, sz) for sy in (-1, 0, 1) for sz in (-1, 0, 1) if (sy, sz) != (0, 0)]
    steps = (-2, -1, 1, 2)

    barrier = pltpu.get_barrier_semaphore()
    for step in steps:
        pl.semaphore_signal(barrier, inc=1, device_id={"gx": at_x(step)}, device_id_type=pl.DeviceIdType.MESH)
    for sy, sz in around:
        pl.semaphore_signal(barrier, inc=1, device_id=at_yz(sy, sz), device_id_type=pl.DeviceIdType.MESH)

    loads = [
        pltpu.make_async_copy(src, dst, load_sem.at[n])
        for n, (src, dst) in enumerate((
            (lw_hbm, lw), (sel_hbm, sel), (ew_hbm, ew), (cw_hbm, cw), (m1_hbm, m1), (m2_hbm, m2),
            (uw_hbm, uw), (dw_hbm, dw), (wide_hbm, wide), (slab_hbm, slab),
        ))
    ]
    for load in loads:
        load.start()

    row_z = lax.broadcasted_iota(jnp.int32, (192, 128), 0) % 16 // 2
    lane_z = lax.broadcasted_iota(jnp.int32, (192, 128), 1) % 8
    keep = row_z == lane_z
    cells = dot(disp[...].reshape(192, 32), place[...])
    own = jnp.zeros((64, 128), F32)
    for jy in range(2):
        part = jnp.where(keep, cells[:, 128 * jy : 128 * jy + 128], 0.0).astype(BF)
        own = own + dot(rows[jy], part)
    layers[8:12] = own.astype(BF).reshape(4, 16, 128)

    pl.semaphore_wait(barrier, 12)
    x_copies = []
    for n, step in enumerate(steps):
        x_copies.append(remote(
            layers.at[8:12], layers.at[pl.ds(8 - 4 * step, 4)], x_send.at[n], x_recv.at[n], gx=at_x(step)
        ))
        x_copies[-1].start()

    for n in (0, 1, 2, 3):
        loads[n].wait()
    w = dot(sel[0], lw[0]) + dot(sel[1], lw[1]) + dot(sel[2], lw[2])
    w = w.reshape(4, 192, 64)
    wl[:, 0:128] = jnp.concatenate([w[0], w[1]], axis=1).astype(BF)
    wl[:, 128:256] = jnp.concatenate([w[2], w[3]], axis=1).astype(BF)

    def pair_tiles(src, a, b):
        taps = [src[9 * a + 3 * b + c].astype(F32) for c in range(3)]
        none = jnp.zeros_like(taps[0])
        for m in range(4):
            lo = taps[m] if m < 3 else none
            hi = taps[m - 1] if m > 0 else none
            yield m, jnp.transpose(jnp.concatenate([lo, hi], axis=0)).astype(BF)

    we[...] = jnp.zeros_like(we)
    wc[...] = jnp.zeros_like(wc)
    for a in range(3):
        for b in range(3):
            for m, tile in pair_tiles(ew, a, b):
                dz, jz = m // 2, m % 2
                for dy in range(2):
                    for jy in range(2):
                        oy = 2 * dy + jy - b
                        if 0 <= oy < 2:
                            row = ((a * 2 + dy) * 2 + dz) * 256 + (jy * 2 + jz) * 64
                            we[row : row + 64, oy * 128 : oy * 128 + 128] = tile
            for m, tile in pair_tiles(cw, a, b):
                dz, jz = m // 2, m % 2
                for dy in range(2):
                    for jy in range(2):
                        oy = 2 * dy + jy - b
                        if 0 <= oy < 2:
                            for s in range(2):
                                row = (((s * 3 + a) * 2 + dy) * 2 + dz) * 256 + (jy * 2 + jz) * 64
                                wc[row : row + 64, oy * 128 : oy * 128 + 128] = tile[s * 64 : s * 64 + 64]

    for copy in x_copies:
        copy.wait_recv()
    quarter = lax.broadcasted_iota(jnp.int32, (16, 128), 1) // 32
    for g in range(5):
        for side in range(2):
            tile = jnp.zeros((16, 128), F32)
            for i in range(4):
                shift = (32 * i + 32 * (1 - side)) % 128
                t = layers[4 * g + i].astype(F32)
                tile = jnp.where(quarter == i, pltpu.roll(t, shift, axis=1) if shift else t, tile)
            slab_out[side, g] = tile.astype(BF)
    n_copies = []
    for n, (sy, sz) in enumerate(around):
        if sy == 0:
            src, dst = layers, left if sz == 1 else right
        else:
            side = 0 if sy == 1 else 1
            src, dst = slab_out.at[side], slab_in.at[side, (0, 1, 2)[sz]]
        n_copies.append(remote(src, dst, n_send.at[n], n_recv.at[n], **at_yz(sy, sz)))
        n_copies[-1].start()

    for n in range(4, 10):
        loads[n].wait()
    wm1[...] = jnp.zeros_like(wm1)
    wm2[...] = jnp.zeros_like(wm2)
    for a in range(3):
        for b in range(3):
            for c in range(3):
                for src, dst in ((m1, wm1), (m2, wm2)):
                    tile = jnp.transpose(src[9 * a + 3 * b + c].astype(F32)).astype(BF)
                    for dy in range(2):
                        for jy in range(2):
                            oy = 2 * dy + jy - b
                            if 0 <= oy < 2:
                                row = ((a * 2 + dy) * 3 + c) * 256 + jy * 128
                                dst[row : row + 128, oy * 128 : oy * 128 + 128] = tile
    wd[...] = dw[...].reshape(2, 256, 128)
    for a in range(2):
        for b in range(2):
            pairs = jnp.concatenate([uw[4 * a + 2 * b + 1], uw[4 * a + 2 * b]], axis=0).astype(F32)
            wu[a, :, b * 128 : b * 128 + 128] = jnp.transpose(pairs).astype(BF)
    wh[...] = jnp.zeros_like(wh)
    for g in range(4):
        wh[3 * g : 3 * g + 3, 64 * g : 64 * g + 64] = hw[...].astype(F32)

    for copy in n_copies:
        copy.wait_recv()
    for n, src in enumerate((layers, left, right)):
        sides[:, 128 * n : 128 * n + 128] = src[...].reshape(320, 128)
        for side in range(2):
            slabs[side, :, 128 * n : 128 * n + 128] = slab_in[side, n].reshape(80, 128)
    mid = dot(sides[...], wide[...]).reshape(20, 16, 256)
    half = lax.broadcasted_iota(jnp.int32, (20, 16, 128), 2) < 64
    first, second = pltpu.roll(mid[:, :, :128], 64, axis=2), pltpu.roll(mid[:, :, 128:], 64, axis=2)
    ends = [dot(slabs[side], slab[...]).reshape(5, 16, 256) for side in range(2)]
    lows, highs = [], []
    for i in range(4):
        lane = 128 * (i // 2)
        low, high = ends[0][:, :, lane : lane + 128], ends[1][:, :, lane : lane + 128]
        lows.append(pltpu.roll(low, 64, axis=2) if i % 2 == 1 else low)
        highs.append(pltpu.roll(high, 64, axis=2) if i % 2 == 0 else high)
    low = jnp.stack(lows, axis=1).reshape(20, 16, 128)
    high = jnp.stack(highs, axis=1).reshape(20, 16, 128)
    qt[:, :, 0:128] = jnp.where(half, low, first)
    qt[:, :, 128:256] = jnp.where(half, first, second)
    qt[:, :, 256:384] = jnp.where(half, second, high)

    @pl.loop(0, 20)
    def _(x):
        q = qt[x]
        for dy in range(2):
            for dz in range(2):
                s = dy * 16 + dz
                r = pltpu.roll(q, 384 - s, axis=1) if s else q
                g = dy * 2 + dz
                patch[x, 16 * g : 16 * g + 16, :] = r.astype(BF)

    @pl.loop(0, 18)
    def _(x):
        p = patch[pl.ds(x, 3)].reshape(192, 384)
        v = lax.dot_general(p, wl[...], (((0,), (0,)), ((), ())), preferred_element_type=F32)
        v = act(v)
        f0[x] = v.astype(BF)
        f1[x] = pltpu.roll(v, 383, axis=0).astype(BF)

    @pl.loop(0, 8)
    def _(i):
        for h in range(2):
            x = 2 * i + h
            taps = []
            for a in range(3):
                for dy in range(2):
                    for src in (f0, f1):
                        taps.append(src[x + a, dy * 16 : dy * 16 + 352, :])
            v = dot(jnp.concatenate(taps, axis=1), we[...])
            skip[x] = act(v).astype(BF)

    @pl.loop(0, 8)
    def _(x):
        lhs = jnp.concatenate([skip[2 * x], skip[2 * x + 1]], axis=1)
        v = act(dot(lhs, wd[...].reshape(512, 128)))
        for c in range(3):
            r = pltpu.roll(v, 352 - c, axis=0) if c else v
            r = r.reshape(11, 2, 16, 128)
            coarse[c, x, :, 0:128] = r[:, 0].reshape(176, 128).astype(BF)
            coarse[c, x, :, 128:256] = r[:, 1].reshape(176, 128).astype(BF)

    @pl.loop(0, 3)
    def _(i):
        for h in range(2):
            x = 2 * i + h
            taps = []
            for a in range(3):
                for dy in range(2):
                    for c in range(3):
                        taps.append(coarse[c, x + a, dy * 16 : dy * 16 + 160, :])
            v = act(dot(jnp.concatenate(taps, axis=1), wm1[...]))
            for c in range(3):
                r = pltpu.roll(v, 160 - c, axis=0) if c else v
                middle[c, x] = r.astype(BF)

    @pl.loop(0, 2)
    def _(i):
        for h in range(2):
            x = 2 * i + h
            taps = []
            for a in range(3):
                for dy in range(2):
                    for c in range(3):
                        taps.append(middle[c, x + a, dy * 16 : dy * 16 + 144, :])
            v = act(dot(jnp.concatenate(taps, axis=1), wm2[...]))
            deep[x] = v.astype(BF)

    low = lax.broadcasted_iota(jnp.int32, (17, 16, 128), 2) < 64

    def spread(dst, f, blocks):
        for dz in range(2):
            r = pltpu.roll(blocks, 15, axis=1) if dz else blocks
            r = r[:, 0:8]
            for dy in range(2):
                dst[dy, dz, f] = r[dy : dy + 16].reshape(128, 256).astype(BF)

    @pl.loop(0, 6)
    def _(f):
        v = skip[f + 5].astype(F32).reshape(22, 16, 256)
        halves = []
        for jy in range(2):
            s = v[2 + jy : 19 + jy, :, 128 - 128 * jy : 256 - 128 * jy]
            t = jnp.where(low, pltpu.roll(s, 13, axis=1), pltpu.roll(s, 14, axis=1))
            halves.append(pltpu.roll(t, 64, axis=2))
        spread(ks, f, jnp.concatenate(halves, axis=2))

    @pl.loop(0, 6)
    def _(f):
        xd = (f + 1) // 2
        a = (f + 1) % 2
        d = deep[xd]
        us = []
        for jy in range(2):
            us.append(act(dot(d[:, jy * 128 : jy * 128 + 128], wu[a])).reshape(9, 1, 16, 256))
        u = jnp.concatenate(us, axis=1).reshape(18, 16, 256)
        halves = []
        for jy in range(2):
            s = u[jy : 17 + jy, :, 128 - 128 * jy : 256 - 128 * jy]
            halves.append(jnp.where(low, s, pltpu.roll(s, 15, axis=1)))
        spread(ku, f, jnp.concatenate(halves, axis=2))

    @pl.loop(0, 2)
    def _(i):
        x = 2 * i
        taps = []
        for src in (ks, ku):
            for a in range(3):
                for dy in range(2):
                    for dz in range(2):
                        taps.append(src[dy, dz, pl.ds(x + a, 2)].reshape(256, 256))
        v = act(dot(jnp.concatenate(taps, axis=1), wc[...])).astype(BF)
        for h in range(2):
            j = v[h * 128 : h * 128 + 128]
            heads[x + h] = lax.dot_general(
                wh[...].astype(BF), j, (((1,), (1,)), ((), ())), preferred_element_type=F32
            )

    h = heads[...].reshape(64, 128)
    coarse_part = h.astype(BF)
    total = disp[...].astype(F32).reshape(192, 32)
    for part in (coarse_part, (h - coarse_part.astype(F32)).astype(BF)):
        for jy in range(2):
            t = lax.dot_general(rows[jy], part, (((0,), (0,)), ((), ())), preferred_element_type=F32)
            t = jnp.where(keep, t, 0.0).astype(BF)
            total = total + lax.dot_general(
                t, place[:, 128 * jy : 128 * jy + 128], (((1,), (1,)), ((), ())), preferred_element_type=F32
            )
    out[...] = total.reshape(3, 4, 16, 32)
    for copy in x_copies + n_copies:
        copy.wait_send()


def local(d, lw, ew, dw, m1, m2, uw, cw, hw):
    wide, slab = widen_lanes()
    vm, anywhere = pl.BlockSpec(memory_space=pltpu.VMEM), pl.BlockSpec(memory_space=pl.ANY)
    out = pl.pallas_call(
        unet,
        out_shape=jax.ShapeDtypeStruct((3, 4, 16, 32), F32),
        in_specs=[vm] * 3 + [anywhere] * 10 + [vm],
        out_specs=vm,
        scratch_shapes=[
            pltpu.VMEM((20, 16, 128), BF),
            pltpu.VMEM((20, 16, 128), BF),
            pltpu.VMEM((20, 16, 128), BF),
            pltpu.VMEM((2, 5, 16, 128), BF),
            pltpu.VMEM((2, 3, 5, 16, 128), BF),
            pltpu.VMEM((320, 384), BF),
            pltpu.VMEM((2, 80, 384), BF),
            pltpu.VMEM((4, 16, 128), F32),
            pltpu.VMEM((20, 16, 384), F32),
            pltpu.VMEM((3, 27, 64), BF),
            pltpu.VMEM((3, 768, 27), BF),
            pltpu.VMEM((384, 256), BF),
            pltpu.VMEM((384, 256), BF),
            pltpu.VMEM((27, 64, 64), BF),
            pltpu.VMEM((8, 64, 128), BF),
            pltpu.VMEM((27, 128, 128), BF),
            pltpu.VMEM((27, 128, 128), BF),
            pltpu.VMEM((8, 64, 128), BF),
            pltpu.VMEM((27, 64, 128), BF),
            pltpu.VMEM((20, 64, 384), BF),
            pltpu.VMEM((192, 256), BF),
            pltpu.VMEM((3072, 256), BF),
            pltpu.VMEM((2, 256, 128), BF),
            pltpu.VMEM((4608, 256), BF),
            pltpu.VMEM((4608, 256), BF),
            pltpu.VMEM((2, 128, 256), BF),
            pltpu.VMEM((6144, 256), BF),
            pltpu.VMEM((16, 256), F32),
            pltpu.VMEM((18, 384, 256), BF),
            pltpu.VMEM((18, 384, 256), BF),
            pltpu.VMEM((16, 352, 256), BF),
            pltpu.VMEM((3, 8, 176, 256), BF),
            pltpu.VMEM((3, 6, 160, 256), BF),
            pltpu.VMEM((4, 144, 256), BF),
            pltpu.VMEM((2, 2, 6, 128, 256), BF),
            pltpu.VMEM((2, 2, 6, 128, 256), BF),
            pltpu.SemaphoreType.DMA((10,)),
            pltpu.SemaphoreType.DMA((4,)),
            pltpu.SemaphoreType.DMA((4,)),
            pltpu.SemaphoreType.DMA((8,)),
            pltpu.SemaphoreType.DMA((8,)),
        ],
        compiler_params=pltpu.CompilerParams(
            vmem_limit_bytes=58 * 1024 * 1024, collective_id=0, has_side_effects=True
        ),
    )(
        jnp.transpose(d, (0, 1, 3, 2)), jnp.asarray(place_columns(), BF), jnp.asarray(gather_rows(), BF),
        jnp.transpose(lw, (2, 0, 1)), jnp.asarray(lift_selection(), BF),
        jnp.asarray(wide, BF), jnp.asarray(slab, BF),
        ew, jnp.transpose(dw, (0, 2, 1)), m1, m2, uw, cw, hw,
    )
    return jnp.transpose(out, (0, 1, 3, 2))


def solution(mesh):
    placed = (P(None, "gx", "gy", "gz"), P(), P(), P(), P(), P(), P(), P(), P())
    return jax.shard_map(
        local, mesh=mesh, in_specs=placed, out_specs=P(None, "gx", "gy", "gz"), check_vma=False
    )
```

```python
import jax
import jax.numpy as jnp
import numpy as np
from jax import lax
from jax.experimental import pallas as pl
from jax.experimental.pallas import tpu as pltpu
from jax.sharding import PartitionSpec as P

BF = jnp.bfloat16
F32 = jnp.float32


def act(v):
    return jnp.where(v > 0, v, 0.1 * v)


def lift_selection():
    sel = np.zeros((3, 4, 192, 27), np.float32)
    for oy in range(2):
        for oz in range(2):
            for dx in range(3):
                for dy in range(2):
                    for dz in range(2):
                        for jy in range(2):
                            for jz in range(2):
                                b, c = 2 * dy + jy - oy, 2 * dz + jz - oz
                                if 0 <= b < 3 and 0 <= c < 3:
                                    for ch in range(3):
                                        row = (((dx * 2 + dy) * 2 + dz) * 16 + (jy * 2 + jz) * 3 + ch)
                                        sel[ch, oy * 2 + oz, row, 9 * dx + 3 * b + c] = 1
    return sel.reshape(3, 768, 27)


def place_columns():
    place = np.zeros((32, 256), np.float32)
    for jy in range(2):
        for lane in range(128):
            place[2 * (lane // 8) + jy, 128 * jy + lane] = 1
    return place


def gather_rows():
    rows = np.zeros((2, 64, 192), np.float32)
    for jy in range(2):
        for x in range(4):
            for z in range(16):
                for c in range(3):
                    rows[jy, 16 * x + jy * 6 + (z % 2) * 3 + c, 64 * c + 16 * x + z] = 1
    return rows


def widen_lanes():
    wide = np.zeros((384, 256), np.float32)
    slab = np.zeros((384, 256), np.float32)
    for piece, (first, shift) in enumerate(((0, 4), (4, -4), (0, 12))):
        for z in range(first, 8 if piece < 2 else 4):
            for y in range(16):
                wide[128 * piece + 8 * y + z, 16 * y + z + shift] = 1
            for i in range(4):
                for y in range(4):
                    slab[128 * piece + 32 * i + 8 * y + z, 64 * i + 16 * y + z + shift] = 1
    return wide, slab


def dot(a, b):
    return jnp.dot(a, b, preferred_element_type=F32)


def remote(src, dst, send, recv, **where):
    return pltpu.make_async_remote_copy(
        src_ref=src, dst_ref=dst, send_sem=send, recv_sem=recv,
        device_id=where, device_id_type=pl.DeviceIdType.MESH,
    )


def unet(
    disp, place, rows, lw_hbm, sel_hbm, wide_hbm, slab_hbm,
    ew_hbm, dw_hbm, m1_hbm, m2_hbm, uw_hbm, cw_hbm, hw,
    out,
    layers, left, right, slab_out, slab_in, sides, slabs, heads, qt,
    lw, sel, wide, slab, ew, dw, m1, m2, uw, cw,
    patch, wl, we, wd, wm1, wm2, wu, wc, wh,
    f0, f1, skip, coarse, middle, deep, ks, ku,
    load_sem, x_send, x_recv, n_send, n_recv,
):
    gx, gy, gz = lax.axis_index("gx"), lax.axis_index("gy"), lax.axis_index("gz")
    nx, ny, nz = lax.axis_size("gx"), lax.axis_size("gy"), lax.axis_size("gz")

    def at_x(step):
        return lax.rem(gx + nx + step, nx)

    def at_yz(sy, sz):
        return {"gy": lax.rem(gy + ny + sy, ny), "gz": lax.rem(gz + nz + sz, nz)}

    around = [(sy, sz) for sy in (-1, 0, 1) for sz in (-1, 0, 1) if (sy, sz) != (0, 0)]
    steps = (-2, -1, 1, 2)

    barrier = pltpu.get_barrier_semaphore()
    for step in steps:
        pl.semaphore_signal(barrier, inc=1, device_id={"gx": at_x(step)}, device_id_type=pl.DeviceIdType.MESH)
    for sy, sz in around:
        pl.semaphore_signal(barrier, inc=1, device_id=at_yz(sy, sz), device_id_type=pl.DeviceIdType.MESH)

    loads = [
        pltpu.make_async_copy(src, dst, load_sem.at[n])
        for n, (src, dst) in enumerate((
            (lw_hbm, lw), (sel_hbm, sel), (ew_hbm, ew), (cw_hbm, cw), (m1_hbm, m1), (m2_hbm, m2),
            (uw_hbm, uw), (dw_hbm, dw), (wide_hbm, wide), (slab_hbm, slab),
        ))
    ]
    for load in loads:
        load.start()

    row_z = lax.broadcasted_iota(jnp.int32, (192, 128), 0) % 16 // 2
    lane_z = lax.broadcasted_iota(jnp.int32, (192, 128), 1) % 8
    keep = row_z == lane_z
    cells = dot(disp[...].reshape(192, 32), place[...])
    own = jnp.zeros((64, 128), F32)
    for jy in range(2):
        part = jnp.where(keep, cells[:, 128 * jy : 128 * jy + 128], 0.0).astype(BF)
        own = own + dot(rows[jy], part)
    layers[8:12] = own.astype(BF).reshape(4, 16, 128)

    pl.semaphore_wait(barrier, 12)
    x_copies = []
    for n, step in enumerate(steps):
        x_copies.append(remote(
            layers.at[8:12], layers.at[pl.ds(8 - 4 * step, 4)], x_send.at[n], x_recv.at[n], gx=at_x(step)
        ))
        x_copies[-1].start()

    for n in (0, 1, 2, 3):
        loads[n].wait()
    w = dot(sel[0], lw[0]) + dot(sel[1], lw[1]) + dot(sel[2], lw[2])
    w = w.reshape(4, 192, 64)
    wl[:, 0:128] = jnp.concatenate([w[0], w[1]], axis=1).astype(BF)
    wl[:, 128:256] = jnp.concatenate([w[2], w[3]], axis=1).astype(BF)

    def pair_tiles(src, a, b):
        taps = [src[9 * a + 3 * b + c].astype(F32) for c in range(3)]
        none = jnp.zeros_like(taps[0])
        for m in range(4):
            lo = taps[m] if m < 3 else none
            hi = taps[m - 1] if m > 0 else none
            yield m, jnp.transpose(jnp.concatenate([lo, hi], axis=0)).astype(BF)

    we[...] = jnp.zeros_like(we)
    wc[...] = jnp.zeros_like(wc)
    for a in range(3):
        for b in range(3):
            for m, tile in pair_tiles(ew, a, b):
                dz, jz = m // 2, m % 2
                for dy in range(2):
                    for jy in range(2):
                        oy = 2 * dy + jy - b
                        if 0 <= oy < 2:
                            row = ((a * 2 + dy) * 2 + dz) * 256 + (jy * 2 + jz) * 64
                            we[row : row + 64, oy * 128 : oy * 128 + 128] = tile
            for m, tile in pair_tiles(cw, a, b):
                dz, jz = m // 2, m % 2
                for dy in range(2):
                    for jy in range(2):
                        oy = 2 * dy + jy - b
                        if 0 <= oy < 2:
                            for s in range(2):
                                row = (((s * 3 + a) * 2 + dy) * 2 + dz) * 256 + (jy * 2 + jz) * 64
                                wc[row : row + 64, oy * 128 : oy * 128 + 128] = tile[s * 64 : s * 64 + 64]

    for copy in x_copies:
        copy.wait_recv()
    quarter = lax.broadcasted_iota(jnp.int32, (16, 128), 1) // 32
    for g in range(5):
        for side in range(2):
            tile = jnp.zeros((16, 128), F32)
            for i in range(4):
                shift = (32 * i + 32 * (1 - side)) % 128
                t = layers[4 * g + i].astype(F32)
                tile = jnp.where(quarter == i, pltpu.roll(t, shift, axis=1) if shift else t, tile)
            slab_out[side, g] = tile.astype(BF)
    n_copies = []
    for n, (sy, sz) in enumerate(around):
        if sy == 0:
            src, dst = layers, left if sz == 1 else right
        else:
            side = 0 if sy == 1 else 1
            src, dst = slab_out.at[side], slab_in.at[side, (0, 1, 2)[sz]]
        n_copies.append(remote(src, dst, n_send.at[n], n_recv.at[n], **at_yz(sy, sz)))
        n_copies[-1].start()

    for n in range(4, 10):
        loads[n].wait()
    wm1[...] = jnp.zeros_like(wm1)
    wm2[...] = jnp.zeros_like(wm2)
    for a in range(3):
        for b in range(3):
            for c in range(3):
                for src, dst in ((m1, wm1), (m2, wm2)):
                    tile = jnp.transpose(src[9 * a + 3 * b + c].astype(F32)).astype(BF)
                    for dy in range(2):
                        for jy in range(2):
                            oy = 2 * dy + jy - b
                            if 0 <= oy < 2:
                                row = ((a * 2 + dy) * 3 + c) * 256 + jy * 128
                                dst[row : row + 128, oy * 128 : oy * 128 + 128] = tile
    wd[...] = dw[...].reshape(2, 256, 128)
    for a in range(2):
        for b in range(2):
            pairs = jnp.concatenate([uw[4 * a + 2 * b + 1], uw[4 * a + 2 * b]], axis=0).astype(F32)
            wu[a, :, b * 128 : b * 128 + 128] = jnp.transpose(pairs).astype(BF)
    wh[...] = jnp.zeros_like(wh)
    for g in range(4):
        wh[3 * g : 3 * g + 3, 64 * g : 64 * g + 64] = hw[...].astype(F32)

    for copy in n_copies:
        copy.wait_recv()
    for n, src in enumerate((layers, left, right)):
        sides[:, 128 * n : 128 * n + 128] = src[...].reshape(320, 128)
        for side in range(2):
            slabs[side, :, 128 * n : 128 * n + 128] = slab_in[side, n].reshape(80, 128)
    mid = dot(sides[...], wide[...]).reshape(20, 16, 256)
    half = lax.broadcasted_iota(jnp.int32, (20, 16, 128), 2) < 64
    first, second = pltpu.roll(mid[:, :, :128], 64, axis=2), pltpu.roll(mid[:, :, 128:], 64, axis=2)
    ends = [dot(slabs[side], slab[...]).reshape(5, 16, 256) for side in range(2)]
    lows, highs = [], []
    for i in range(4):
        lane = 128 * (i // 2)
        low, high = ends[0][:, :, lane : lane + 128], ends[1][:, :, lane : lane + 128]
        lows.append(pltpu.roll(low, 64, axis=2) if i % 2 == 1 else low)
        highs.append(pltpu.roll(high, 64, axis=2) if i % 2 == 0 else high)
    low = jnp.stack(lows, axis=1).reshape(20, 16, 128)
    high = jnp.stack(highs, axis=1).reshape(20, 16, 128)
    qt[:, :, 0:128] = jnp.where(half, low, first)
    qt[:, :, 128:256] = jnp.where(half, first, second)
    qt[:, :, 256:384] = jnp.where(half, second, high)

    def lay_patch(x):
        q = qt[x]
        for dy in range(2):
            for dz in range(2):
                s = dy * 16 + dz
                r = pltpu.roll(q, 384 - s, axis=1) if s else q
                g = dy * 2 + dz
                patch[x, 16 * g : 16 * g + 16, :] = r.astype(BF)

    def lift(x):
        p = patch[x : x + 3].reshape(192, 384)
        v = lax.dot_general(p, wl[...], (((0,), (0,)), ((), ())), preferred_element_type=F32)
        v = act(v)
        f0[x] = v.astype(BF)
        f1[x] = pltpu.roll(v, 383, axis=0).astype(BF)

    def encode(x):
        taps = []
        for a in range(3):
            for dy in range(2):
                for src in (f0, f1):
                    taps.append(src[x + a, dy * 16 : dy * 16 + 352, :])
        v = dot(jnp.concatenate(taps, axis=1), we[...])
        skip[x] = act(v).astype(BF)

    def downward(x):
        lhs = jnp.concatenate([skip[2 * x], skip[2 * x + 1]], axis=1)
        v = act(dot(lhs, wd[...].reshape(512, 128)))
        for c in range(3):
            r = pltpu.roll(v, 352 - c, axis=0) if c else v
            r = r.reshape(11, 2, 16, 128)
            coarse[c, x, :, 0:128] = r[:, 0].reshape(176, 128).astype(BF)
            coarse[c, x, :, 128:256] = r[:, 1].reshape(176, 128).astype(BF)

    def conv_half(src, x, size, weight):
        taps = []
        for a in range(3):
            for dy in range(2):
                for c in range(3):
                    taps.append(src[c, x + a, dy * 16 : dy * 16 + size, :])
        return act(dot(jnp.concatenate(taps, axis=1), weight[...]))

    def conv_first(x):
        v = conv_half(coarse, x, 160, wm1)
        for c in range(3):
            r = pltpu.roll(v, 160 - c, axis=0) if c else v
            middle[c, x] = r.astype(BF)

    def conv_second(x):
        deep[x] = conv_half(middle, x, 144, wm2).astype(BF)

    low = lax.broadcasted_iota(jnp.int32, (17, 16, 128), 2) < 64

    def spread(dst, f, blocks):
        for dz in range(2):
            r = pltpu.roll(blocks, 15, axis=1) if dz else blocks
            r = r[:, 0:8]
            for dy in range(2):
                dst[dy, dz, f] = r[dy : dy + 16].reshape(128, 256).astype(BF)

    def spread_skip(f):
        v = skip[f + 5].astype(F32).reshape(22, 16, 256)
        halves = []
        for jy in range(2):
            s = v[2 + jy : 19 + jy, :, 128 - 128 * jy : 256 - 128 * jy]
            t = jnp.where(low, pltpu.roll(s, 13, axis=1), pltpu.roll(s, 14, axis=1))
            halves.append(pltpu.roll(t, 64, axis=2))
        spread(ks, f, jnp.concatenate(halves, axis=2))

    def upsample(f):
        xd = (f + 1) // 2
        a = (f + 1) % 2
        d = deep[xd]
        us = []
        for jy in range(2):
            us.append(act(dot(d[:, jy * 128 : jy * 128 + 128], wu[a])).reshape(9, 1, 16, 256))
        u = jnp.concatenate(us, axis=1).reshape(18, 16, 256)
        halves = []
        for jy in range(2):
            s = u[jy : 17 + jy, :, 128 - 128 * jy : 256 - 128 * jy]
            halves.append(jnp.where(low, s, pltpu.roll(s, 15, axis=1)))
        spread(ku, f, jnp.concatenate(halves, axis=2))

    def decode(x, n):
        taps = []
        for src in (ks, ku):
            for a in range(3):
                for dy in range(2):
                    for dz in range(2):
                        taps.append(src[dy, dz, x + a : x + a + n].reshape(128 * n, 256))
        v = act(dot(jnp.concatenate(taps, axis=1), wc[...])).astype(BF)
        for h in range(n):
            heads[x + h] = lax.dot_general(
                wh[...].astype(BF), v[h * 128 : h * 128 + 128], (((1,), (1,)), ((), ())), preferred_element_type=F32
            )

    for x in range(20):
        lay_patch(x)
    for x in range(3):
        lift(x)
    for x in range(16):
        if x + 3 < 18:
            lift(x + 3)
        encode(x)
        if x % 2 == 1 and x > 1:
            downward(x // 2 - 1)
    spread_skip(0)
    downward(7)
    for x in range(6):
        conv_first(x)
        if x:
            spread_skip(x)
    for x in range(4):
        conv_second(x)
        for f in range(6):
            if (f + 1) // 2 == x - 1:
                upsample(f)
    upsample(5)
    decode(0, 2)
    decode(2, 2)

    h = heads[...].reshape(64, 128)
    coarse_part = h.astype(BF)
    total = disp[...].astype(F32).reshape(192, 32)
    for part in (coarse_part, (h - coarse_part.astype(F32)).astype(BF)):
        for jy in range(2):
            t = lax.dot_general(rows[jy], part, (((0,), (0,)), ((), ())), preferred_element_type=F32)
            t = jnp.where(keep, t, 0.0).astype(BF)
            total = total + lax.dot_general(
                t, place[:, 128 * jy : 128 * jy + 128], (((1,), (1,)), ((), ())), preferred_element_type=F32
            )
    out[...] = total.reshape(3, 4, 16, 32)
    for copy in x_copies + n_copies:
        copy.wait_send()


def local(d, lw, ew, dw, m1, m2, uw, cw, hw):
    wide, slab = widen_lanes()
    vm, anywhere = pl.BlockSpec(memory_space=pltpu.VMEM), pl.BlockSpec(memory_space=pl.ANY)
    out = pl.pallas_call(
        unet,
        out_shape=jax.ShapeDtypeStruct((3, 4, 16, 32), F32),
        in_specs=[vm] * 3 + [anywhere] * 10 + [vm],
        out_specs=vm,
        scratch_shapes=[
            pltpu.VMEM((20, 16, 128), BF),
            pltpu.VMEM((20, 16, 128), BF),
            pltpu.VMEM((20, 16, 128), BF),
            pltpu.VMEM((2, 5, 16, 128), BF),
            pltpu.VMEM((2, 3, 5, 16, 128), BF),
            pltpu.VMEM((320, 384), BF),
            pltpu.VMEM((2, 80, 384), BF),
            pltpu.VMEM((4, 16, 128), F32),
            pltpu.VMEM((20, 16, 384), F32),
            pltpu.VMEM((3, 27, 64), BF),
            pltpu.VMEM((3, 768, 27), BF),
            pltpu.VMEM((384, 256), BF),
            pltpu.VMEM((384, 256), BF),
            pltpu.VMEM((27, 64, 64), BF),
            pltpu.VMEM((8, 64, 128), BF),
            pltpu.VMEM((27, 128, 128), BF),
            pltpu.VMEM((27, 128, 128), BF),
            pltpu.VMEM((8, 64, 128), BF),
            pltpu.VMEM((27, 64, 128), BF),
            pltpu.VMEM((20, 64, 384), BF),
            pltpu.VMEM((192, 256), BF),
            pltpu.VMEM((3072, 256), BF),
            pltpu.VMEM((2, 256, 128), BF),
            pltpu.VMEM((4608, 256), BF),
            pltpu.VMEM((4608, 256), BF),
            pltpu.VMEM((2, 128, 256), BF),
            pltpu.VMEM((6144, 256), BF),
            pltpu.VMEM((16, 256), F32),
            pltpu.VMEM((18, 384, 256), BF),
            pltpu.VMEM((18, 384, 256), BF),
            pltpu.VMEM((16, 352, 256), BF),
            pltpu.VMEM((3, 8, 176, 256), BF),
            pltpu.VMEM((3, 6, 160, 256), BF),
            pltpu.VMEM((4, 144, 256), BF),
            pltpu.VMEM((2, 2, 6, 128, 256), BF),
            pltpu.VMEM((2, 2, 6, 128, 256), BF),
            pltpu.SemaphoreType.DMA((10,)),
            pltpu.SemaphoreType.DMA((4,)),
            pltpu.SemaphoreType.DMA((4,)),
            pltpu.SemaphoreType.DMA((8,)),
            pltpu.SemaphoreType.DMA((8,)),
        ],
        compiler_params=pltpu.CompilerParams(
            vmem_limit_bytes=58 * 1024 * 1024, collective_id=0, has_side_effects=True
        ),
    )(
        jnp.transpose(d, (0, 1, 3, 2)), jnp.asarray(place_columns(), BF), jnp.asarray(gather_rows(), BF),
        jnp.transpose(lw, (2, 0, 1)), jnp.asarray(lift_selection(), BF),
        jnp.asarray(wide, BF), jnp.asarray(slab, BF),
        ew, jnp.transpose(dw, (0, 2, 1)), m1, m2, uw, cw, hw,
    )
    return jnp.transpose(out, (0, 1, 3, 2))


def solution(mesh):
    placed = (P(None, "gx", "gy", "gz"), P(), P(), P(), P(), P(), P(), P(), P())
    return jax.shard_map(
        local, mesh=mesh, in_specs=placed, out_specs=P(None, "gx", "gy", "gz"), check_vma=False
    )
```

```python
import jax
import jax.numpy as jnp
import numpy as np
from jax import lax
from jax.experimental import pallas as pl
from jax.experimental.pallas import tpu as pltpu
from jax.sharding import PartitionSpec as P

BF = jnp.bfloat16
F32 = jnp.float32


def act(v):
    return jnp.where(v > 0, v, 0.1 * v)


def lift_selection():
    sel = np.zeros((3, 4, 192, 27), np.float32)
    for oy in range(2):
        for oz in range(2):
            for dx in range(3):
                for dy in range(2):
                    for dz in range(2):
                        for jy in range(2):
                            for jz in range(2):
                                b, c = 2 * dy + jy - oy, 2 * dz + jz - oz
                                if 0 <= b < 3 and 0 <= c < 3:
                                    for ch in range(3):
                                        row = (((dx * 2 + dy) * 2 + dz) * 16 + (jy * 2 + jz) * 3 + ch)
                                        sel[ch, oy * 2 + oz, row, 9 * dx + 3 * b + c] = 1
    return sel.reshape(3, 768, 27)


def place_columns():
    place = np.zeros((32, 256), np.float32)
    for jy in range(2):
        for lane in range(128):
            place[2 * (lane // 8) + jy, 128 * jy + lane] = 1
    return place


def gather_rows():
    rows = np.zeros((2, 64, 192), np.float32)
    for jy in range(2):
        for x in range(4):
            for z in range(16):
                for c in range(3):
                    rows[jy, 16 * x + jy * 6 + (z % 2) * 3 + c, 64 * c + 16 * x + z] = 1
    return rows


def widen_lanes():
    wide = np.zeros((384, 256), np.float32)
    for piece, (first, last, shift) in enumerate(((0, 8, 4), (4, 8, -4), (0, 4, 12))):
        for z in range(first, last):
            for y in range(16):
                wide[128 * piece + 8 * y + z, 16 * y + z + shift] = 1
    return wide


def dot(a, b):
    return jnp.dot(a, b, preferred_element_type=F32)


def remote(src, dst, send, recv, **where):
    return pltpu.make_async_remote_copy(
        src_ref=src, dst_ref=dst, send_sem=send, recv_sem=recv,
        device_id=where, device_id_type=pl.DeviceIdType.MESH,
    )


def unet(
    disp_hbm, place_hbm, rows_hbm, lw_hbm, sel_hbm, ew_hbm, cw_hbm, wide_hbm,
    m1_hbm, m2_hbm, uw_hbm, dw_hbm, hw_hbm,
    out,
    disp, place, rows, lw, sel, ew, cw, wide, m1, m2, uw, dw, hw,
    layers, left, right, slab_out, slab_in, sides, heads, mid,
    patch, edge, wl, we, wd, wm1, wm2, wu, wc, wh,
    f0, f1, skip, coarse, middle, deep, ks, ku,
    load_sem, x_send, x_recv, z_send, z_recv, y_send, y_recv,
):
    gx, gy, gz = lax.axis_index("gx"), lax.axis_index("gy"), lax.axis_index("gz")
    nx, ny, nz = lax.axis_size("gx"), lax.axis_size("gy"), lax.axis_size("gz")

    def at_x(step):
        return {"gx": lax.rem(gx + nx + step, nx)}

    def at_y(step):
        return {"gy": lax.rem(gy + ny + step, ny)}

    def at_z(step):
        return {"gz": lax.rem(gz + nz + step, nz)}

    steps = (-2, -1, 1, 2)
    barrier = pltpu.get_barrier_semaphore()
    for where in [at_x(step) for step in steps] + [at_y(-1), at_y(1), at_z(-1), at_z(1)]:
        pl.semaphore_signal(barrier, inc=1, device_id=where, device_id_type=pl.DeviceIdType.MESH)

    loads = [
        pltpu.make_async_copy(src, dst, load_sem.at[n])
        for n, (src, dst) in enumerate((
            (disp_hbm, disp), (place_hbm, place), (rows_hbm, rows),
            (lw_hbm, lw), (sel_hbm, sel), (ew_hbm, ew), (cw_hbm, cw), (wide_hbm, wide),
            (m1_hbm, m1), (m2_hbm, m2), (uw_hbm, uw), (dw_hbm, dw), (hw_hbm, hw),
        ))
    ]
    for load in loads:
        load.start()
    for load in loads[:3]:
        load.wait()

    row_z = lax.broadcasted_iota(jnp.int32, (192, 128), 0) % 16 // 2
    lane_z = lax.broadcasted_iota(jnp.int32, (192, 128), 1) % 8
    keep = row_z == lane_z
    cells = dot(disp[...].reshape(192, 32), place[...])
    own = jnp.zeros((64, 128), F32)
    for jy in range(2):
        part = jnp.where(keep, cells[:, 128 * jy : 128 * jy + 128], 0.0).astype(BF)
        own = own + dot(rows[jy], part)
    layers[8:12] = own.astype(BF).reshape(4, 16, 128)

    pl.semaphore_wait(barrier, 8)
    x_copies = []
    for n, step in enumerate(steps):
        x_copies.append(remote(
            layers.at[8:12], layers.at[pl.ds(8 - 4 * step, 4)], x_send.at[n], x_recv.at[n], **at_x(step)
        ))
        x_copies[-1].start()

    for load in loads[3:7]:
        load.wait()
    w = dot(sel[0], lw[0]) + dot(sel[1], lw[1]) + dot(sel[2], lw[2])
    w = w.reshape(4, 192, 64)
    wl[:, 0:128] = jnp.concatenate([w[0], w[1]], axis=1).astype(BF)
    wl[:, 128:256] = jnp.concatenate([w[2], w[3]], axis=1).astype(BF)

    def pair_tiles(src, a, b):
        taps = [src[9 * a + 3 * b + c].astype(F32) for c in range(3)]
        none = jnp.zeros_like(taps[0])
        for m in range(4):
            lo = taps[m] if m < 3 else none
            hi = taps[m - 1] if m > 0 else none
            yield m, jnp.transpose(jnp.concatenate([lo, hi], axis=0)).astype(BF)

    we[...] = jnp.zeros_like(we)
    wc[...] = jnp.zeros_like(wc)
    for a in range(3):
        for b in range(3):
            for m, tile in pair_tiles(ew, a, b):
                dz, jz = m // 2, m % 2
                for dy in range(2):
                    for jy in range(2):
                        oy = 2 * dy + jy - b
                        if 0 <= oy < 2:
                            row = ((a * 2 + dy) * 2 + dz) * 256 + (jy * 2 + jz) * 64
                            we[row : row + 64, oy * 128 : oy * 128 + 128] = tile
            for m, tile in pair_tiles(cw, a, b):
                dz, jz = m // 2, m % 2
                for dy in range(2):
                    for jy in range(2):
                        oy = 2 * dy + jy - b
                        if 0 <= oy < 2:
                            for s in range(2):
                                row = (((s * 3 + a) * 2 + dy) * 2 + dz) * 256 + (jy * 2 + jz) * 64
                                wc[row : row + 64, oy * 128 : oy * 128 + 128] = tile[s * 64 : s * 64 + 64]

    for copy in x_copies:
        copy.wait_recv()
    z_copies = [
        remote(layers, left, z_send.at[0], z_recv.at[0], **at_z(1)),
        remote(layers, right, z_send.at[1], z_recv.at[1], **at_z(-1)),
    ]
    for copy in z_copies:
        copy.start()

    for load in loads[7:]:
        load.wait()
    wm1[...] = jnp.zeros_like(wm1)
    wm2[...] = jnp.zeros_like(wm2)
    for a in range(3):
        for b in range(3):
            for c in range(3):
                for src, dst in ((m1, wm1), (m2, wm2)):
                    tile = jnp.transpose(src[9 * a + 3 * b + c].astype(F32)).astype(BF)
                    for dy in range(2):
                        for jy in range(2):
                            oy = 2 * dy + jy - b
                            if 0 <= oy < 2:
                                row = ((a * 2 + dy) * 3 + c) * 256 + jy * 128
                                dst[row : row + 128, oy * 128 : oy * 128 + 128] = tile
    wd[...] = dw[...].reshape(2, 256, 128)
    for a in range(2):
        for b in range(2):
            pairs = jnp.concatenate([uw[4 * a + 2 * b + 1], uw[4 * a + 2 * b]], axis=0).astype(F32)
            wu[a, :, b * 128 : b * 128 + 128] = jnp.transpose(pairs).astype(BF)
    wh[...] = jnp.zeros_like(wh)
    for g in range(4):
        wh[3 * g : 3 * g + 3, 64 * g : 64 * g + 64] = hw[...].astype(F32)

    for copy in z_copies:
        copy.wait_recv()
    for n, src in enumerate((layers, left, right)):
        sides[:, 128 * n : 128 * n + 128] = src[...].reshape(320, 128)
    mid[...] = dot(sides[...], wide[...]).reshape(20, 16, 256)
    half = lax.broadcasted_iota(jnp.int32, (10, 16, 128), 2) < 64
    pairs = mid[...].reshape(10, 2, 16, 256)
    upper = jnp.where(half, pltpu.roll(pairs[:, 0, :, 128:], 64, axis=2), pairs[:, 1, :, 128:])
    lower = jnp.where(half, pairs[:, 0, :, :128], pltpu.roll(pairs[:, 1, :, :128], 64, axis=2))
    slab_out[0] = upper.astype(BF)
    slab_out[1] = lower.astype(BF)
    y_copies = [
        remote(slab_out.at[0], slab_in.at[0], y_send.at[0], y_recv.at[0], **at_y(1)),
        remote(slab_out.at[1], slab_in.at[1], y_send.at[1], y_recv.at[1], **at_y(-1)),
    ]
    for copy in y_copies:
        copy.start()

    def lay_inner(x):
        q = mid[x]
        for dy in range(2):
            for dz in range(2):
                shift = dy * 16 + dz
                r = pltpu.roll(q, 256 - shift, axis=1) if shift else q
                g = dy * 2 + dz
                patch[x, 16 * g : 16 * g + 16, :] = r.astype(BF)

    lane = lax.broadcasted_iota(jnp.int32, (16, 128), 1)

    def lay_outer(x):
        first, last = mid[x, :, 0:128], mid[x, :, 128:256]
        low, high = slab_in[0, x // 2].astype(F32), slab_in[1, x // 2].astype(F32)
        if x % 2:
            low, high = pltpu.roll(low, 64, axis=1), pltpu.roll(high, 64, axis=1)
        one = jnp.where(lane < 64, low, jnp.where(lane < 80, pltpu.roll(last, 80, axis=1), pltpu.roll(high, 80, axis=1)))
        two = jnp.where(lane < 48, pltpu.roll(low, 112, axis=1), jnp.where(lane < 64, pltpu.roll(first, 48, axis=1), pltpu.roll(high, 64, axis=1)))
        for dy, q in enumerate((one, two)):
            for dz in range(2):
                r = pltpu.roll(q, 127, axis=1) if dz else q
                g = dy * 2 + dz
                edge[x, 16 * g : 16 * g + 16, :] = r.astype(BF)

    def lift(src, x, size):
        p = src[x : x + 3].reshape(192, size)
        v = lax.dot_general(p, wl[...], (((0,), (0,)), ((), ())), preferred_element_type=F32)
        return act(v)

    def lift_inner(x):
        v = lift(patch, x, 256)
        f0[x, 64:304] = v[:240].astype(BF)
        f1[x, 64:304] = pltpu.roll(v, 255, axis=0)[:240].astype(BF)

    def lift_outer(x):
        v = lift(edge, x, 128)
        for dst, r in ((f0, v), (f1, pltpu.roll(v, 127, axis=0))):
            dst[x, 0:64] = r[:64].astype(BF)
            dst[x, 304:368] = r[64:].astype(BF)

    def encode(x, n, spans):
        taps = []
        for a in range(3):
            for dy in range(2):
                for src in (f0, f1):
                    taps.append(jnp.concatenate(
                        [src[x + a + h, r + dy * 16 : r + dy * 16 + size, :] for h in range(n) for r, size in spans], axis=0
                    ))
        v = act(dot(jnp.concatenate(taps, axis=1), we[...])).astype(BF)
        at = 0
        for h in range(n):
            for r, size in spans:
                skip[x + h, r : r + size] = v[at : at + size]
                at += size

    def downward(x):
        lhs = jnp.concatenate([skip[2 * x], skip[2 * x + 1]], axis=1)
        v = act(dot(lhs, wd[...].reshape(512, 128)))
        for c in range(3):
            r = pltpu.roll(v, 352 - c, axis=0) if c else v
            r = r.reshape(11, 2, 16, 128)
            coarse[c, x, :, 0:128] = r[:, 0].reshape(176, 128).astype(BF)
            coarse[c, x, :, 128:256] = r[:, 1].reshape(176, 128).astype(BF)

    def conv_half(src, x, size, weight):
        taps = []
        for a in range(3):
            for dy in range(2):
                for c in range(3):
                    taps.append(src[c, x + a, dy * 16 : dy * 16 + size, :])
        return act(dot(jnp.concatenate(taps, axis=1), weight[...]))

    def conv_first(x):
        v = conv_half(coarse, x, 160, wm1)
        for c in range(3):
            r = pltpu.roll(v, 160 - c, axis=0) if c else v
            middle[c, x] = r.astype(BF)

    def conv_second(x):
        deep[x] = conv_half(middle, x, 144, wm2).astype(BF)

    low = lax.broadcasted_iota(jnp.int32, (17, 16, 128), 2) < 64

    def spread(dst, f, blocks):
        for dz in range(2):
            r = pltpu.roll(blocks, 15, axis=1) if dz else blocks
            r = r[:, 0:8]
            for dy in range(2):
                dst[dy, dz, f] = r[dy : dy + 16].reshape(128, 256).astype(BF)

    def spread_skip(f):
        v = skip[f + 5].astype(F32).reshape(22, 16, 256)
        halves = []
        for jy in range(2):
            s = v[2 + jy : 19 + jy, :, 128 - 128 * jy : 256 - 128 * jy]
            t = jnp.where(low, pltpu.roll(s, 13, axis=1), pltpu.roll(s, 14, axis=1))
            halves.append(pltpu.roll(t, 64, axis=2))
        spread(ks, f, jnp.concatenate(halves, axis=2))

    def upsample(f):
        xd = (f + 1) // 2
        a = (f + 1) % 2
        d = deep[xd]
        us = []
        for jy in range(2):
            us.append(act(dot(d[:, jy * 128 : jy * 128 + 128], wu[a])).reshape(9, 1, 16, 256))
        u = jnp.concatenate(us, axis=1).reshape(18, 16, 256)
        halves = []
        for jy in range(2):
            s = u[jy : 17 + jy, :, 128 - 128 * jy : 256 - 128 * jy]
            halves.append(jnp.where(low, s, pltpu.roll(s, 15, axis=1)))
        spread(ku, f, jnp.concatenate(halves, axis=2))

    def decode(x, n):
        taps = []
        for src in (ks, ku):
            for a in range(3):
                for dy in range(2):
                    for dz in range(2):
                        taps.append(src[dy, dz, x + a : x + a + n].reshape(128 * n, 256))
        v = act(dot(jnp.concatenate(taps, axis=1), wc[...])).astype(BF)
        for h in range(n):
            heads[x + h] = lax.dot_general(
                wh[...].astype(BF), v[h * 128 : h * 128 + 128], (((1,), (1,)), ((), ())), preferred_element_type=F32
            )

    for x in range(20):
        lay_inner(x)
    for x in range(4):
        lift_inner(x)
    for x in range(0, 16, 2):
        for h in range(2):
            if x + 4 + h < 18:
                lift_inner(x + 4 + h)
        encode(x, 2, ((64, 224),))
    for copy in y_copies:
        copy.wait_recv()
    for x in range(20):
        lay_outer(x)
    for x in range(6):
        lift_outer(x)
    for x in range(0, 16, 4):
        for h in range(4):
            if x + 6 + h < 18:
                lift_outer(x + 6 + h)
        encode(x, 4, ((0, 64), (288, 64)))
        if x:
            downward(x // 2 - 2)
            downward(x // 2 - 1)
    downward(6)
    spread_skip(0)
    downward(7)
    for x in range(6):
        conv_first(x)
        if x:
            spread_skip(x)
    for x in range(4):
        conv_second(x)
        for f in range(6):
            if (f + 1) // 2 == x - 1:
                upsample(f)
    upsample(5)
    decode(0, 2)
    decode(2, 2)

    h = heads[...].reshape(64, 128)
    coarse_part = h.astype(BF)
    total = jnp.zeros((192, 32), F32)
    for part in (coarse_part, (h - coarse_part.astype(F32)).astype(BF)):
        for jy in range(2):
            t = lax.dot_general(rows[jy], part, (((0,), (0,)), ((), ())), preferred_element_type=F32)
            t = jnp.where(keep, t, 0.0).astype(BF)
            total = total + lax.dot_general(
                t, place[:, 128 * jy : 128 * jy + 128], (((1,), (1,)), ((), ())), preferred_element_type=F32
            )
    out[...] = total.reshape(3, 4, 16, 32)
    for copy in x_copies + z_copies + y_copies:
        copy.wait_send()


def local(d, lw, ew, dw, m1, m2, uw, cw, hw):
    anywhere = pl.BlockSpec(memory_space=pl.ANY)
    args = (
        jnp.transpose(d, (0, 1, 3, 2)), jnp.asarray(place_columns(), BF), jnp.asarray(gather_rows(), BF),
        jnp.transpose(lw, (2, 0, 1)), jnp.asarray(lift_selection(), BF), ew, cw, jnp.asarray(widen_lanes(), BF),
        m1, m2, uw, jnp.transpose(dw, (0, 2, 1)), hw,
    )
    out = pl.pallas_call(
        unet,
        out_shape=jax.ShapeDtypeStruct((3, 4, 16, 32), F32),
        in_specs=[anywhere] * 13,
        out_specs=pl.BlockSpec(memory_space=pltpu.VMEM),
        scratch_shapes=[pltpu.VMEM(arg.shape, arg.dtype) for arg in args] + [
            pltpu.VMEM((20, 16, 128), BF),
            pltpu.VMEM((20, 16, 128), BF),
            pltpu.VMEM((20, 16, 128), BF),
            pltpu.VMEM((2, 10, 16, 128), BF),
            pltpu.VMEM((2, 10, 16, 128), BF),
            pltpu.VMEM((320, 384), BF),
            pltpu.VMEM((4, 16, 128), F32),
            pltpu.VMEM((20, 16, 256), F32),
            pltpu.VMEM((20, 64, 256), BF),
            pltpu.VMEM((20, 64, 128), BF),
            pltpu.VMEM((192, 256), BF),
            pltpu.VMEM((3072, 256), BF),
            pltpu.VMEM((2, 256, 128), BF),
            pltpu.VMEM((4608, 256), BF),
            pltpu.VMEM((4608, 256), BF),
            pltpu.VMEM((2, 128, 256), BF),
            pltpu.VMEM((6144, 256), BF),
            pltpu.VMEM((16, 256), F32),
            pltpu.VMEM((18, 368, 256), BF),
            pltpu.VMEM((18, 368, 256), BF),
            pltpu.VMEM((16, 352, 256), BF),
            pltpu.VMEM((3, 8, 176, 256), BF),
            pltpu.VMEM((3, 6, 160, 256), BF),
            pltpu.VMEM((4, 144, 256), BF),
            pltpu.VMEM((2, 2, 6, 128, 256), BF),
            pltpu.VMEM((2, 2, 6, 128, 256), BF),
            pltpu.SemaphoreType.DMA((13,)),
            pltpu.SemaphoreType.DMA((4,)),
            pltpu.SemaphoreType.DMA((4,)),
            pltpu.SemaphoreType.DMA((2,)),
            pltpu.SemaphoreType.DMA((2,)),
            pltpu.SemaphoreType.DMA((2,)),
            pltpu.SemaphoreType.DMA((2,)),
        ],
        compiler_params=pltpu.CompilerParams(
            vmem_limit_bytes=58 * 1024 * 1024, collective_id=0, has_side_effects=True
        ),
    )(*args)
    return d.astype(F32) + jnp.transpose(out, (0, 1, 3, 2))


def solution(mesh):
    placed = (P(None, "gx", "gy", "gz"), P(), P(), P(), P(), P(), P(), P(), P())
    return jax.shard_map(
        local, mesh=mesh, in_specs=placed, out_specs=P(None, "gx", "gy", "gz"), check_vma=False
    )
```

```python
import jax
import jax.numpy as jnp
import numpy as np
from jax import lax
from jax.experimental import pallas as pl
from jax.experimental.pallas import tpu as pltpu
from jax.sharding import PartitionSpec as P

BF = jnp.bfloat16
F32 = jnp.float32


def act(v):
    return jnp.where(v > 0, v, 0.1 * v)


def lift_selection():
    sel = np.zeros((3, 4, 192, 27), np.float32)
    for oy in range(2):
        for oz in range(2):
            for dx in range(3):
                for dy in range(2):
                    for dz in range(2):
                        for jy in range(2):
                            for jz in range(2):
                                b, c = 2 * dy + jy - oy, 2 * dz + jz - oz
                                if 0 <= b < 3 and 0 <= c < 3:
                                    for ch in range(3):
                                        row = (((dx * 2 + dy) * 2 + dz) * 16 + (jy * 2 + jz) * 3 + ch)
                                        sel[ch, oy * 2 + oz, row, 9 * dx + 3 * b + c] = 1
    return sel.reshape(3, 768, 27)


def place_columns():
    place = np.zeros((32, 256), np.float32)
    for jy in range(2):
        for lane in range(128):
            place[2 * (lane // 8) + jy, 128 * jy + lane] = 1
    return place


def gather_rows():
    rows = np.zeros((2, 64, 192), np.float32)
    for jy in range(2):
        for x in range(4):
            for z in range(16):
                for c in range(3):
                    rows[jy, 16 * x + jy * 6 + (z % 2) * 3 + c, 64 * c + 16 * x + z] = 1
    return rows


def spread_head():
    spread = np.zeros((96, 16), np.float32)
    for jy in range(2):
        for k in range(3):
            for z in range(16):
                spread[48 * jy + 16 * k + z, jy * 6 + (z % 2) * 3 + k] = 1
    return spread


def widen_lanes():
    wide = np.zeros((384, 256), np.float32)
    for piece, (first, last, shift) in enumerate(((0, 8, 4), (4, 8, -4), (0, 4, 12))):
        for z in range(first, last):
            for y in range(16):
                wide[128 * piece + 8 * y + z, 16 * y + z + shift] = 1
    return wide


def dot(a, b):
    return jnp.dot(a, b, preferred_element_type=F32)


def remote(src, dst, send, recv, **where):
    return pltpu.make_async_remote_copy(
        src_ref=src, dst_ref=dst, send_sem=send, recv_sem=recv,
        device_id=where, device_id_type=pl.DeviceIdType.MESH,
    )


def unet(
    disp_hbm, place_hbm, rows_hbm, lw_hbm, sel_hbm, ew_hbm, cw_hbm, wide_hbm,
    m1_hbm, m2_hbm, uw_hbm, dw_hbm, hw_hbm, spr_hbm,
    out,
    disp, place, rows, lw, sel, ew, cw, wide, m1, m2, uw, dw, hw, spr,
    layers, left, right, slab_out, slab_in, sides, whs, mid,
    patch, edge, wl, we, wd, wm1, wm2, wu, wc, wh,
    f0, f1, skip, coarse, middle, deep, ks, ku,
    load_sem, x_send, x_recv, z_send, z_recv, y_send, y_recv,
):
    gx, gy, gz = lax.axis_index("gx"), lax.axis_index("gy"), lax.axis_index("gz")
    nx, ny, nz = lax.axis_size("gx"), lax.axis_size("gy"), lax.axis_size("gz")

    def at_x(step):
        return {"gx": lax.rem(gx + nx + step, nx)}

    def at_y(step):
        return {"gy": lax.rem(gy + ny + step, ny)}

    def at_z(step):
        return {"gz": lax.rem(gz + nz + step, nz)}

    steps = (-2, -1, 1, 2)
    barrier = pltpu.get_barrier_semaphore()
    for where in [at_x(step) for step in steps] + [at_y(-1), at_y(1), at_z(-1), at_z(1)]:
        pl.semaphore_signal(barrier, inc=1, device_id=where, device_id_type=pl.DeviceIdType.MESH)

    loads = [
        pltpu.make_async_copy(src, dst, load_sem.at[n])
        for n, (src, dst) in enumerate((
            (disp_hbm, disp), (place_hbm, place), (rows_hbm, rows),
            (lw_hbm, lw), (sel_hbm, sel), (ew_hbm, ew), (cw_hbm, cw), (wide_hbm, wide),
            (m1_hbm, m1), (m2_hbm, m2), (uw_hbm, uw), (dw_hbm, dw), (hw_hbm, hw), (spr_hbm, spr),
        ))
    ]
    for load in loads:
        load.start()
    for load in loads[:3]:
        load.wait()

    row_z = lax.broadcasted_iota(jnp.int32, (192, 128), 0) % 16 // 2
    lane_z = lax.broadcasted_iota(jnp.int32, (192, 128), 1) % 8
    keep = row_z == lane_z
    cells = dot(disp[...].reshape(192, 32), place[...])
    own = jnp.zeros((64, 128), F32)
    for jy in range(2):
        part = jnp.where(keep, cells[:, 128 * jy : 128 * jy + 128], 0.0).astype(BF)
        own = own + dot(rows[jy], part)
    layers[8:12] = own.astype(BF).reshape(4, 16, 128)

    pl.semaphore_wait(barrier, 8)
    x_copies = []
    for n, step in enumerate(steps):
        x_copies.append(remote(
            layers.at[8:12], layers.at[pl.ds(8 - 4 * step, 4)], x_send.at[n], x_recv.at[n], **at_x(step)
        ))
        x_copies[-1].start()

    for load in loads[3:7]:
        load.wait()
    w = dot(sel[0], lw[0]) + dot(sel[1], lw[1]) + dot(sel[2], lw[2])
    w = w.reshape(4, 192, 64)
    wl[:, 0:128] = jnp.concatenate([w[0], w[1]], axis=1).astype(BF)
    wl[:, 128:256] = jnp.concatenate([w[2], w[3]], axis=1).astype(BF)

    def pair_tiles(src, a, b):
        taps = [src[9 * a + 3 * b + c].astype(F32) for c in range(3)]
        none = jnp.zeros_like(taps[0])
        for m in range(4):
            lo = taps[m] if m < 3 else none
            hi = taps[m - 1] if m > 0 else none
            yield m, jnp.transpose(jnp.concatenate([lo, hi], axis=0)).astype(BF)

    we[...] = jnp.zeros_like(we)
    wc[...] = jnp.zeros_like(wc)
    for a in range(3):
        for b in range(3):
            for m, tile in pair_tiles(ew, a, b):
                dz, jz = m // 2, m % 2
                for dy in range(2):
                    for jy in range(2):
                        oy = 2 * dy + jy - b
                        if 0 <= oy < 2:
                            row = ((a * 2 + dy) * 2 + dz) * 256 + (jy * 2 + jz) * 64
                            we[row : row + 64, oy * 128 : oy * 128 + 128] = tile
            for m, tile in pair_tiles(cw, a, b):
                dz, jz = m // 2, m % 2
                for dy in range(2):
                    for jy in range(2):
                        oy = 2 * dy + jy - b
                        if 0 <= oy < 2:
                            for s in range(2):
                                row = (((s * 3 + a) * 2 + dy) * 2 + dz) * 256 + (jy * 2 + jz) * 64
                                wc[row : row + 64, oy * 128 : oy * 128 + 128] = tile[s * 64 : s * 64 + 64]

    for copy in x_copies:
        copy.wait_recv()
    z_copies = [
        remote(layers, left, z_send.at[0], z_recv.at[0], **at_z(1)),
        remote(layers, right, z_send.at[1], z_recv.at[1], **at_z(-1)),
    ]
    for copy in z_copies:
        copy.start()

    for load in loads[7:]:
        load.wait()
    wm1[...] = jnp.zeros_like(wm1)
    wm2[...] = jnp.zeros_like(wm2)
    for a in range(3):
        for b in range(3):
            for c in range(3):
                for src, dst in ((m1, wm1), (m2, wm2)):
                    tile = jnp.transpose(src[9 * a + 3 * b + c].astype(F32)).astype(BF)
                    for dy in range(2):
                        for jy in range(2):
                            oy = 2 * dy + jy - b
                            if 0 <= oy < 2:
                                row = ((a * 2 + dy) * 3 + c) * 256 + jy * 128
                                dst[row : row + 128, oy * 128 : oy * 128 + 128] = tile
    wd[...] = dw[...].reshape(2, 256, 128)
    for a in range(2):
        for b in range(2):
            pairs = jnp.concatenate([uw[4 * a + 2 * b + 1], uw[4 * a + 2 * b]], axis=0).astype(F32)
            wu[a, :, b * 128 : b * 128 + 128] = jnp.transpose(pairs).astype(BF)
    wh[...] = jnp.zeros_like(wh)
    for g in range(4):
        wh[3 * g : 3 * g + 3, 64 * g : 64 * g + 64] = hw[...].astype(F32)
    whs[...] = dot(spr[...], wh[...].astype(BF)).astype(BF)

    for copy in z_copies:
        copy.wait_recv()
    for n, src in enumerate((layers, left, right)):
        sides[:, 128 * n : 128 * n + 128] = src[...].reshape(320, 128)
    mid[...] = dot(sides[...], wide[...]).reshape(20, 16, 256)
    half = lax.broadcasted_iota(jnp.int32, (10, 16, 128), 2) < 64
    pairs = mid[...].reshape(10, 2, 16, 256)
    upper = jnp.where(half, pltpu.roll(pairs[:, 0, :, 128:], 64, axis=2), pairs[:, 1, :, 128:])
    lower = jnp.where(half, pairs[:, 0, :, :128], pltpu.roll(pairs[:, 1, :, :128], 64, axis=2))
    slab_out[0] = upper.astype(BF)
    slab_out[1] = lower.astype(BF)
    y_copies = [
        remote(slab_out.at[0], slab_in.at[0], y_send.at[0], y_recv.at[0], **at_y(1)),
        remote(slab_out.at[1], slab_in.at[1], y_send.at[1], y_recv.at[1], **at_y(-1)),
    ]
    for copy in y_copies:
        copy.start()

    def lay_inner(x):
        q = mid[x]
        for dy in range(2):
            for dz in range(2):
                shift = dy * 16 + dz
                r = pltpu.roll(q, 256 - shift, axis=1) if shift else q
                g = dy * 2 + dz
                patch[x, 16 * g : 16 * g + 16, :] = r.astype(BF)

    lane = lax.broadcasted_iota(jnp.int32, (16, 128), 1)

    def lay_outer(x):
        first, last = mid[x, :, 0:128], mid[x, :, 128:256]
        low, high = slab_in[0, x // 2].astype(F32), slab_in[1, x // 2].astype(F32)
        if x % 2:
            low, high = pltpu.roll(low, 64, axis=1), pltpu.roll(high, 64, axis=1)
        one = jnp.where(lane < 64, low, jnp.where(lane < 80, pltpu.roll(last, 80, axis=1), pltpu.roll(high, 80, axis=1)))
        two = jnp.where(lane < 48, pltpu.roll(low, 112, axis=1), jnp.where(lane < 64, pltpu.roll(first, 48, axis=1), pltpu.roll(high, 64, axis=1)))
        for dy, q in enumerate((one, two)):
            for dz in range(2):
                r = pltpu.roll(q, 127, axis=1) if dz else q
                g = dy * 2 + dz
                edge[x, 16 * g : 16 * g + 16, :] = r.astype(BF)

    def lift(src, x, size):
        p = src[x : x + 3].reshape(192, size)
        v = lax.dot_general(p, wl[...], (((0,), (0,)), ((), ())), preferred_element_type=F32)
        return act(v)

    def lift_inner(x):
        v = lift(patch, x, 256)
        f0[x, 64:304] = v[:240].astype(BF)
        f1[x, 64:304] = pltpu.roll(v, 255, axis=0)[:240].astype(BF)

    def lift_outer(x):
        v = lift(edge, x, 128)
        for dst, r in ((f0, v), (f1, pltpu.roll(v, 127, axis=0))):
            dst[x, 0:64] = r[:64].astype(BF)
            dst[x, 304:368] = r[64:].astype(BF)

    def encode(x, n, spans):
        taps = []
        for a in range(3):
            for dy in range(2):
                for src in (f0, f1):
                    taps.append(jnp.concatenate(
                        [src[x + a + h, r + dy * 16 : r + dy * 16 + size, :] for h in range(n) for r, size in spans], axis=0
                    ))
        v = act(dot(jnp.concatenate(taps, axis=1), we[...])).astype(BF)
        at = 0
        for h in range(n):
            for r, size in spans:
                skip[x + h, r : r + size] = v[at : at + size]
                at += size

    def downward(x):
        lhs = jnp.concatenate([skip[2 * x], skip[2 * x + 1]], axis=1)
        v = act(dot(lhs, wd[...].reshape(512, 128)))
        for c in range(3):
            r = pltpu.roll(v, 352 - c, axis=0) if c else v
            r = r.reshape(11, 2, 16, 128)
            coarse[c, x, :, 0:128] = r[:, 0].reshape(176, 128).astype(BF)
            coarse[c, x, :, 128:256] = r[:, 1].reshape(176, 128).astype(BF)

    def conv_half(src, x, size, weight):
        taps = []
        for a in range(3):
            for dy in range(2):
                for c in range(3):
                    taps.append(src[c, x + a, dy * 16 : dy * 16 + size, :])
        return act(dot(jnp.concatenate(taps, axis=1), weight[...]))

    def conv_first(x):
        v = conv_half(coarse, x, 160, wm1)
        for c in range(3):
            r = pltpu.roll(v, 160 - c, axis=0) if c else v
            middle[c, x] = r.astype(BF)

    def conv_second(x):
        deep[x] = conv_half(middle, x, 144, wm2).astype(BF)

    low = lax.broadcasted_iota(jnp.int32, (17, 16, 128), 2) < 64

    def spread(dst, f, blocks):
        for dz in range(2):
            r = pltpu.roll(blocks, 15, axis=1) if dz else blocks
            r = r[:, 0:8]
            for dy in range(2):
                dst[dy, dz, f] = r[dy : dy + 16].reshape(128, 256).astype(BF)

    def spread_skip(f):
        v = skip[f + 5].astype(F32).reshape(22, 16, 256)
        halves = []
        for jy in range(2):
            s = v[2 + jy : 19 + jy, :, 128 - 128 * jy : 256 - 128 * jy]
            t = jnp.where(low, pltpu.roll(s, 13, axis=1), pltpu.roll(s, 14, axis=1))
            halves.append(pltpu.roll(t, 64, axis=2))
        spread(ks, f, jnp.concatenate(halves, axis=2))

    def upsample(f):
        xd = (f + 1) // 2
        a = (f + 1) % 2
        d = deep[xd]
        us = []
        for jy in range(2):
            us.append(act(dot(d[:, jy * 128 : jy * 128 + 128], wu[a])).reshape(9, 1, 16, 256))
        u = jnp.concatenate(us, axis=1).reshape(18, 16, 256)
        halves = []
        for jy in range(2):
            s = u[jy : 17 + jy, :, 128 - 128 * jy : 256 - 128 * jy]
            halves.append(jnp.where(low, s, pltpu.roll(s, 15, axis=1)))
        spread(ku, f, jnp.concatenate(halves, axis=2))

    def decode(x, n):
        taps = []
        for src in (ks, ku):
            for a in range(3):
                for dy in range(2):
                    for dz in range(2):
                        taps.append(src[dy, dz, x + a : x + a + n].reshape(128 * n, 256))
        return act(dot(jnp.concatenate(taps, axis=1), wc[...])).astype(BF)

    for x in range(6):
        lay_inner(x)
    for x in range(4):
        lift_inner(x)
    for x in range(0, 16, 2):
        if x == 14:
            for copy in y_copies:
                copy.wait_recv()
            for h in range(8):
                lay_outer(h)
            for h in range(6):
                lift_outer(h)
        for h in range(2):
            if x + 6 + h < 20:
                lay_inner(x + 6 + h)
            if x + 4 + h < 18:
                lift_inner(x + 4 + h)
        encode(x, 1, ((64, 224),))
        encode(x + 1, 1, ((64, 224),))
    for x in range(0, 16, 4):
        for h in range(4):
            if x + 8 + h < 20:
                lay_outer(x + 8 + h)
            if x + 6 + h < 18:
                lift_outer(x + 6 + h)
        encode(x, 2, ((0, 64), (288, 64)))
        encode(x + 2, 2, ((0, 64), (288, 64)))
        if x:
            downward(x // 2 - 2)
            downward(x // 2 - 1)
    downward(6)
    spread_skip(0)
    downward(7)
    for x in range(6):
        conv_first(x)
        if x:
            spread_skip(x)
    for x in range(4):
        conv_second(x)
        for f in range(6):
            if (f + 1) // 2 == x - 1:
                upsample(f)
    upsample(5)
    v = jnp.concatenate([decode(x, 1) for x in range(4)], axis=0)

    h = lax.dot_general(whs[...], v, (((1,), (1,)), ((), ())), preferred_element_type=F32)
    spot = lax.broadcasted_iota(jnp.int32, (96, 512), 0) % 16 // 2 == lax.broadcasted_iota(jnp.int32, (96, 512), 1) % 8
    h = jnp.where(spot, h, 0.0)
    rough = h.astype(BF)
    fine = (h - rough.astype(F32)).astype(BF)
    sums = []
    for part in (rough, fine):
        wide_part = jnp.concatenate([
            jnp.concatenate([part[48 * jy : 48 * jy + 48, 128 * x : 128 * x + 128] for x in range(4)], axis=0)
            for jy in range(2)
        ], axis=1)
        sums.append(lax.dot_general(wide_part, place[...], (((1,), (1,)), ((), ())), preferred_element_type=F32))
    total = (sums[0] + sums[1]).reshape(4, 3, 16, 32)
    for x in range(4):
        out[:, x] = total[x]
    for copy in x_copies + z_copies + y_copies:
        copy.wait_send()


def local(d, lw, ew, dw, m1, m2, uw, cw, hw):
    anywhere = pl.BlockSpec(memory_space=pltpu.HBM)
    args = (
        jnp.transpose(d, (0, 1, 3, 2)), jnp.asarray(place_columns(), BF), jnp.asarray(gather_rows(), BF),
        jnp.transpose(lw, (2, 0, 1)), jnp.asarray(lift_selection(), BF), ew, cw, jnp.asarray(widen_lanes(), BF),
        m1, m2, uw, jnp.transpose(dw, (0, 2, 1)), hw, jnp.asarray(spread_head(), BF),
    )
    out = pl.pallas_call(
        unet,
        out_shape=jax.ShapeDtypeStruct((3, 4, 16, 32), F32),
        in_specs=[anywhere] * 14,
        out_specs=pl.BlockSpec(memory_space=pltpu.VMEM),
        scratch_shapes=[pltpu.VMEM(arg.shape, arg.dtype) for arg in args] + [
            pltpu.VMEM((20, 16, 128), BF),
            pltpu.VMEM((20, 16, 128), BF),
            pltpu.VMEM((20, 16, 128), BF),
            pltpu.VMEM((2, 10, 16, 128), BF),
            pltpu.VMEM((2, 10, 16, 128), BF),
            pltpu.VMEM((320, 384), BF),
            pltpu.VMEM((96, 256), BF),
            pltpu.VMEM((20, 16, 256), F32),
            pltpu.VMEM((20, 64, 256), BF),
            pltpu.VMEM((20, 64, 128), BF),
            pltpu.VMEM((192, 256), BF),
            pltpu.VMEM((3072, 256), BF),
            pltpu.VMEM((2, 256, 128), BF),
            pltpu.VMEM((4608, 256), BF),
            pltpu.VMEM((4608, 256), BF),
            pltpu.VMEM((2, 128, 256), BF),
            pltpu.VMEM((6144, 256), BF),
            pltpu.VMEM((16, 256), F32),
            pltpu.VMEM((18, 368, 256), BF),
            pltpu.VMEM((18, 368, 256), BF),
            pltpu.VMEM((16, 352, 256), BF),
            pltpu.VMEM((3, 8, 176, 256), BF),
            pltpu.VMEM((3, 6, 160, 256), BF),
            pltpu.VMEM((4, 144, 256), BF),
            pltpu.VMEM((2, 2, 6, 128, 256), BF),
            pltpu.VMEM((2, 2, 6, 128, 256), BF),
            pltpu.SemaphoreType.DMA((14,)),
            pltpu.SemaphoreType.DMA((4,)),
            pltpu.SemaphoreType.DMA((4,)),
            pltpu.SemaphoreType.DMA((2,)),
            pltpu.SemaphoreType.DMA((2,)),
            pltpu.SemaphoreType.DMA((2,)),
            pltpu.SemaphoreType.DMA((2,)),
        ],
        compiler_params=pltpu.CompilerParams(
            vmem_limit_bytes=58 * 1024 * 1024, collective_id=0, has_side_effects=True
        ),
    )(*args)
    return d.astype(F32) + jnp.transpose(out, (0, 1, 3, 2))


def solution(mesh):
    placed = (P(None, "gx", "gy", "gz"), P(), P(), P(), P(), P(), P(), P(), P())
    return jax.shard_map(
        local, mesh=mesh, in_specs=placed, out_specs=P(None, "gx", "gy", "gz"), check_vma=False
    )
```

```python
import jax
import jax.numpy as jnp
import numpy as np
from jax import lax
from jax.experimental import pallas as pl
from jax.experimental.pallas import tpu as pltpu
from jax.sharding import PartitionSpec as P

BF = jnp.bfloat16
F32 = jnp.float32


def act(v):
    return jnp.where(v > 0, v, 0.1 * v)


def lift_selection():
    sel = np.zeros((3, 4, 192, 27), np.float32)
    for oy in range(2):
        for oz in range(2):
            for dx in range(3):
                for dy in range(2):
                    for dz in range(2):
                        for jy in range(2):
                            for jz in range(2):
                                b, c = 2 * dy + jy - oy, 2 * dz + jz - oz
                                if 0 <= b < 3 and 0 <= c < 3:
                                    for ch in range(3):
                                        row = (((dx * 2 + dy) * 2 + dz) * 16 + (jy * 2 + jz) * 3 + ch)
                                        sel[ch, oy * 2 + oz, row, 9 * dx + 3 * b + c] = 1
    return sel.reshape(3, 768, 27)


def place_columns():
    place = np.zeros((32, 256), np.float32)
    for jy in range(2):
        for lane in range(128):
            place[2 * (lane // 8) + jy, 128 * jy + lane] = 1
    return place


def gather_rows():
    rows = np.zeros((2, 64, 192), np.float32)
    for jy in range(2):
        for x in range(4):
            for z in range(16):
                for c in range(3):
                    rows[jy, 16 * x + jy * 6 + (z % 2) * 3 + c, 64 * c + 16 * x + z] = 1
    return rows


def spread_head():
    spread = np.zeros((96, 16), np.float32)
    for jy in range(2):
        for k in range(3):
            for z in range(16):
                spread[48 * jy + 16 * k + z, jy * 6 + (z % 2) * 3 + k] = 1
    return spread


def widen_lanes():
    wide = np.zeros((384, 256), np.float32)
    for piece, (first, last, shift) in enumerate(((0, 8, 4), (4, 8, -4), (0, 4, 12))):
        for z in range(first, last):
            for y in range(16):
                wide[128 * piece + 8 * y + z, 16 * y + z + shift] = 1
    return wide


def dot(a, b):
    return jnp.dot(a, b, preferred_element_type=F32)


def remote(src, dst, send, recv, **where):
    return pltpu.make_async_remote_copy(
        src_ref=src, dst_ref=dst, send_sem=send, recv_sem=recv,
        device_id=where, device_id_type=pl.DeviceIdType.MESH,
    )


def unet(
    disp_hbm, place_hbm, rows_hbm, lw_hbm, sel_hbm, ew_hbm, cw_hbm, wide_hbm,
    m1_hbm, m2_hbm, uw_hbm, dw_hbm, hw_hbm, spr_hbm,
    out,
    disp, place, rows, lw, sel, ew, cw, wide, m1, m2, uw, dw, hw, spr,
    layers, left, right, slab_out, slab_in, sides, whs, mid,
    patch, edge, wl, we, wd, wm1, wm2, wu, wc, wh,
    f0, f1, skip, coarse, middle, deep, ks, ku,
    load_sem, x_send, x_recv, z_send, z_recv, y_send, y_recv,
):
    gx, gy, gz = lax.axis_index("gx"), lax.axis_index("gy"), lax.axis_index("gz")
    nx, ny, nz = lax.axis_size("gx"), lax.axis_size("gy"), lax.axis_size("gz")

    def at_x(step):
        return {"gx": lax.rem(gx + nx + step, nx)}

    def at_y(step):
        return {"gy": lax.rem(gy + ny + step, ny)}

    def at_z(step):
        return {"gz": lax.rem(gz + nz + step, nz)}

    steps = (-2, -1, 1, 2)
    barrier = pltpu.get_barrier_semaphore()
    for where in [at_x(step) for step in steps] + [at_y(-1), at_y(1), at_z(-1), at_z(1)]:
        pl.semaphore_signal(barrier, inc=1, device_id=where, device_id_type=pl.DeviceIdType.MESH)

    loads = [
        pltpu.make_async_copy(src, dst, load_sem.at[n])
        for n, (src, dst) in enumerate((
            (disp_hbm, disp), (place_hbm, place), (rows_hbm, rows),
            (lw_hbm, lw), (sel_hbm, sel), (ew_hbm, ew), (cw_hbm, cw), (wide_hbm, wide),
            (m1_hbm, m1), (m2_hbm, m2), (uw_hbm, uw), (dw_hbm, dw), (hw_hbm, hw), (spr_hbm, spr),
        ))
    ]
    for load in loads:
        load.start()
    for load in loads[:3]:
        load.wait()

    row_z = lax.broadcasted_iota(jnp.int32, (192, 128), 0) % 16 // 2
    lane_z = lax.broadcasted_iota(jnp.int32, (192, 128), 1) % 8
    keep = row_z == lane_z
    cells = dot(disp[...].reshape(192, 32), place[...])
    own = jnp.zeros((64, 128), F32)
    for jy in range(2):
        part = jnp.where(keep, cells[:, 128 * jy : 128 * jy + 128], 0.0).astype(BF)
        own = own + dot(rows[jy], part)
    layers[8:12] = own.astype(BF).reshape(4, 16, 128)

    pl.semaphore_wait(barrier, 8)
    x_copies = []
    for n, step in enumerate(steps):
        x_copies.append(remote(
            layers.at[8:12], layers.at[pl.ds(8 - 4 * step, 4)], x_send.at[n], x_recv.at[n], **at_x(step)
        ))
        x_copies[-1].start()

    for load in loads[3:7]:
        load.wait()
    w = dot(sel[0], lw[0]) + dot(sel[1], lw[1]) + dot(sel[2], lw[2])
    w = w.reshape(4, 192, 64)
    wl[:, 0:128] = jnp.concatenate([w[0], w[1]], axis=1).astype(BF)
    wl[:, 128:256] = jnp.concatenate([w[2], w[3]], axis=1).astype(BF)

    def pair_tiles(src, a, b):
        taps = [src[9 * a + 3 * b + c].astype(F32) for c in range(3)]
        none = jnp.zeros_like(taps[0])
        for m in range(4):
            lo = taps[m] if m < 3 else none
            hi = taps[m - 1] if m > 0 else none
            yield m, jnp.transpose(jnp.concatenate([lo, hi], axis=0)).astype(BF)

    we[...] = jnp.zeros_like(we)
    wc[...] = jnp.zeros_like(wc)
    for a in range(3):
        for b in range(3):
            for m, tile in pair_tiles(ew, a, b):
                dz, jz = m // 2, m % 2
                for dy in range(2):
                    for jy in range(2):
                        oy = 2 * dy + jy - b
                        if 0 <= oy < 2:
                            row = ((a * 2 + dy) * 2 + dz) * 256 + (jy * 2 + jz) * 64
                            we[row : row + 64, oy * 128 : oy * 128 + 128] = tile
            for m, tile in pair_tiles(cw, a, b):
                dz, jz = m // 2, m % 2
                for dy in range(2):
                    for jy in range(2):
                        oy = 2 * dy + jy - b
                        if 0 <= oy < 2:
                            for s in range(2):
                                row = (((s * 3 + a) * 2 + dy) * 2 + dz) * 256 + (jy * 2 + jz) * 64
                                wc[row : row + 64, oy * 128 : oy * 128 + 128] = tile[s * 64 : s * 64 + 64]

    for copy in x_copies:
        copy.wait_recv()
    z_copies = [
        remote(layers, left, z_send.at[0], z_recv.at[0], **at_z(1)),
        remote(layers, right, z_send.at[1], z_recv.at[1], **at_z(-1)),
    ]
    for copy in z_copies:
        copy.start()

    for load in loads[7:]:
        load.wait()
    wm1[...] = jnp.zeros_like(wm1)
    wm2[...] = jnp.zeros_like(wm2)
    for a in range(3):
        for b in range(3):
            for c in range(3):
                for src, dst in ((m1, wm1), (m2, wm2)):
                    tile = jnp.transpose(src[9 * a + 3 * b + c].astype(F32)).astype(BF)
                    for dy in range(2):
                        for jy in range(2):
                            oy = 2 * dy + jy - b
                            if 0 <= oy < 2:
                                row = ((a * 2 + dy) * 3 + c) * 256 + jy * 128
                                dst[row : row + 128, oy * 128 : oy * 128 + 128] = tile
    wd[...] = dw[...].reshape(2, 256, 128)
    for a in range(2):
        for b in range(2):
            pairs = jnp.concatenate([uw[4 * a + 2 * b + 1], uw[4 * a + 2 * b]], axis=0).astype(F32)
            wu[a, :, b * 128 : b * 128 + 128] = jnp.transpose(pairs).astype(BF)
    wh[...] = jnp.zeros_like(wh)
    for g in range(4):
        wh[3 * g : 3 * g + 3, 64 * g : 64 * g + 64] = hw[...].astype(F32)
    whs[...] = dot(spr[...], wh[...].astype(BF)).astype(BF)

    for copy in z_copies:
        copy.wait_recv()
    for n, src in enumerate((layers, left, right)):
        sides[:, 128 * n : 128 * n + 128] = src[...].reshape(320, 128)
    mid[...] = dot(sides[...], wide[...]).reshape(20, 16, 256)
    half = lax.broadcasted_iota(jnp.int32, (10, 16, 128), 2) < 64
    pairs = mid[...].reshape(10, 2, 16, 256)
    upper = jnp.where(half, pltpu.roll(pairs[:, 0, :, 128:], 64, axis=2), pairs[:, 1, :, 128:])
    lower = jnp.where(half, pairs[:, 0, :, :128], pltpu.roll(pairs[:, 1, :, :128], 64, axis=2))
    slab_out[0] = upper.astype(BF)
    slab_out[1] = lower.astype(BF)
    y_copies = [
        remote(slab_out.at[0], slab_in.at[0], y_send.at[0], y_recv.at[0], **at_y(1)),
        remote(slab_out.at[1], slab_in.at[1], y_send.at[1], y_recv.at[1], **at_y(-1)),
    ]
    for copy in y_copies:
        copy.start()

    def lay_inner(x):
        q = mid[x]
        for dy in range(2):
            for dz in range(2):
                shift = dy * 16 + dz
                r = pltpu.roll(q, 256 - shift, axis=1) if shift else q
                g = dy * 2 + dz
                patch[x, 16 * g : 16 * g + 16, :] = r.astype(BF)

    lane = lax.broadcasted_iota(jnp.int32, (16, 128), 1)

    def lay_outer(x):
        first, last = mid[x, :, 0:128], mid[x, :, 128:256]
        low, high = slab_in[0, x // 2].astype(F32), slab_in[1, x // 2].astype(F32)
        if x % 2:
            low, high = pltpu.roll(low, 64, axis=1), pltpu.roll(high, 64, axis=1)
        one = jnp.where(lane < 64, low, jnp.where(lane < 80, pltpu.roll(last, 80, axis=1), pltpu.roll(high, 80, axis=1)))
        two = jnp.where(lane < 48, pltpu.roll(low, 112, axis=1), jnp.where(lane < 64, pltpu.roll(first, 48, axis=1), pltpu.roll(high, 64, axis=1)))
        for dy, q in enumerate((one, two)):
            for dz in range(2):
                r = pltpu.roll(q, 127, axis=1) if dz else q
                g = dy * 2 + dz
                edge[x, 16 * g : 16 * g + 16, :] = r.astype(BF)

    def lift(src, x, size):
        p = src[x : x + 3].reshape(192, size)
        v = lax.dot_general(p, wl[...], (((0,), (0,)), ((), ())), preferred_element_type=F32)
        return act(v)

    def lift_inner(x):
        v = lift(patch, x, 256)
        f0[x, 64:304] = v[:240].astype(BF)
        f1[x, 64:304] = pltpu.roll(v, 255, axis=0)[:240].astype(BF)

    def lift_outer(x):
        v = lift(edge, x, 128)
        for dst, r in ((f0, v), (f1, pltpu.roll(v, 127, axis=0))):
            dst[x, 0:64] = r[:64].astype(BF)
            dst[x, 304:368] = r[64:].astype(BF)

    def encode(x, n, spans):
        taps = []
        for a in range(3):
            for dy in range(2):
                for src in (f0, f1):
                    taps.append(jnp.concatenate(
                        [src[x + a + h, r + dy * 16 : r + dy * 16 + size, :] for h in range(n) for r, size in spans], axis=0
                    ))
        v = act(dot(jnp.concatenate(taps, axis=1), we[...])).astype(BF)
        at = 0
        for h in range(n):
            for r, size in spans:
                skip[x + h, r : r + size] = v[at : at + size]
                at += size

    def downward(x):
        lhs = jnp.concatenate([skip[2 * x], skip[2 * x + 1]], axis=1)
        v = act(dot(lhs, wd[...].reshape(512, 128)))
        for c in range(3):
            r = pltpu.roll(v, 352 - c, axis=0) if c else v
            r = r.reshape(11, 2, 16, 128)
            coarse[c, x, :, 0:128] = r[:, 0].reshape(176, 128).astype(BF)
            coarse[c, x, :, 128:256] = r[:, 1].reshape(176, 128).astype(BF)

    def conv_half(src, x, size, weight):
        taps = []
        for a in range(3):
            for dy in range(2):
                for c in range(3):
                    taps.append(src[c, x + a, dy * 16 : dy * 16 + size, :])
        return act(dot(jnp.concatenate(taps, axis=1), weight[...]))

    def conv_first(x):
        v = conv_half(coarse, x, 160, wm1)
        for c in range(3):
            r = pltpu.roll(v, 160 - c, axis=0) if c else v
            middle[c, x] = r.astype(BF)

    def conv_second(x):
        deep[x] = conv_half(middle, x, 144, wm2).astype(BF)

    low = lax.broadcasted_iota(jnp.int32, (17, 16, 128), 2) < 64

    def spread(dst, f, blocks):
        for dz in range(2):
            r = pltpu.roll(blocks, 15, axis=1) if dz else blocks
            r = r[:, 0:8]
            for dy in range(2):
                dst[dy, dz, f] = r[dy : dy + 16].reshape(128, 256).astype(BF)

    def spread_skip(f):
        v = skip[f + 5].astype(F32).reshape(22, 16, 256)
        halves = []
        for jy in range(2):
            s = v[2 + jy : 19 + jy, :, 128 - 128 * jy : 256 - 128 * jy]
            t = jnp.where(low, pltpu.roll(s, 13, axis=1), pltpu.roll(s, 14, axis=1))
            halves.append(pltpu.roll(t, 64, axis=2))
        spread(ks, f, jnp.concatenate(halves, axis=2))

    def upsample(f):
        xd = (f + 1) // 2
        a = (f + 1) % 2
        d = deep[xd]
        us = []
        for jy in range(2):
            us.append(act(dot(d[:, jy * 128 : jy * 128 + 128], wu[a])).reshape(9, 1, 16, 256))
        u = jnp.concatenate(us, axis=1).reshape(18, 16, 256)
        halves = []
        for jy in range(2):
            s = u[jy : 17 + jy, :, 128 - 128 * jy : 256 - 128 * jy]
            halves.append(jnp.where(low, s, pltpu.roll(s, 15, axis=1)))
        spread(ku, f, jnp.concatenate(halves, axis=2))

    def decode(x, n):
        taps = []
        for src in (ks, ku):
            for a in range(3):
                for dy in range(2):
                    for dz in range(2):
                        taps.append(src[dy, dz, x + a : x + a + n].reshape(128 * n, 256))
        return act(dot(jnp.concatenate(taps, axis=1), wc[...])).astype(BF)

    for x in range(6):
        lay_inner(x)
    for x in range(4):
        lift_inner(x)
    for x in range(0, 16, 2):
        if x == 14:
            for copy in y_copies:
                copy.wait_recv()
            for h in range(8):
                lay_outer(h)
            for h in range(6):
                lift_outer(h)
        for h in range(2):
            if x + 6 + h < 20:
                lay_inner(x + 6 + h)
            if x + 4 + h < 18:
                lift_inner(x + 4 + h)
        encode(x, 1, ((64, 224),))
        encode(x + 1, 1, ((64, 224),))
    for x in range(0, 16, 4):
        for h in range(4):
            if x + 8 + h < 20:
                lay_outer(x + 8 + h)
            if x + 6 + h < 18:
                lift_outer(x + 6 + h)
        encode(x, 2, ((0, 64), (288, 64)))
        encode(x + 2, 2, ((0, 64), (288, 64)))
        if x:
            downward(x // 2 - 2)
            downward(x // 2 - 1)
    downward(6)
    spread_skip(0)
    downward(7)
    for x in range(6):
        conv_first(x)
        if x:
            spread_skip(x)
    for x in range(4):
        conv_second(x)
        for f in range(6):
            if (f + 1) // 2 == x - 1:
                upsample(f)
    upsample(5)
    v = jnp.concatenate([decode(x, 1) for x in range(4)], axis=0)

    h = lax.dot_general(whs[...], v, (((1,), (1,)), ((), ())), preferred_element_type=F32)
    spot = lax.broadcasted_iota(jnp.int32, (96, 512), 0) % 16 // 2 == lax.broadcasted_iota(jnp.int32, (96, 512), 1) % 8
    h = jnp.where(spot, h, 0.0)
    rough = h.astype(BF)
    fine = (h - rough.astype(F32)).astype(BF)
    sums = []
    for part in (rough, fine):
        wide_part = jnp.concatenate([
            jnp.concatenate([part[48 * jy : 48 * jy + 48, 128 * x : 128 * x + 128] for x in range(4)], axis=0)
            for jy in range(2)
        ], axis=1)
        sums.append(lax.dot_general(wide_part, place[...], (((1,), (1,)), ((), ())), preferred_element_type=F32))
    total = (sums[0] + sums[1]).reshape(4, 3, 16, 32)
    for x in range(4):
        out[:, x] = total[x]
    for copy in x_copies + z_copies + y_copies:
        copy.wait_send()


def local(d, lw, ew, dw, m1, m2, uw, cw, hw):
    anywhere = pl.BlockSpec(memory_space=pltpu.HBM)
    args = (
        jnp.transpose(d, (0, 1, 3, 2)), jnp.asarray(place_columns(), BF), jnp.asarray(gather_rows(), BF),
        jnp.transpose(lw, (2, 0, 1)), jnp.asarray(lift_selection(), BF), ew, cw, jnp.asarray(widen_lanes(), BF),
        m1, m2, uw, jnp.transpose(dw, (0, 2, 1)), hw, jnp.asarray(spread_head(), BF),
    )
    out = pl.pallas_call(
        unet,
        out_shape=pltpu.VMEM((3, 4, 16, 32), F32),
        in_specs=[anywhere] * 14,
        out_specs=pl.BlockSpec(memory_space=pltpu.VMEM),
        scratch_shapes=[pltpu.VMEM(arg.shape, arg.dtype) for arg in args] + [
            pltpu.VMEM((20, 16, 128), BF),
            pltpu.VMEM((20, 16, 128), BF),
            pltpu.VMEM((20, 16, 128), BF),
            pltpu.VMEM((2, 10, 16, 128), BF),
            pltpu.VMEM((2, 10, 16, 128), BF),
            pltpu.VMEM((320, 384), BF),
            pltpu.VMEM((96, 256), BF),
            pltpu.VMEM((20, 16, 256), F32),
            pltpu.VMEM((20, 64, 256), BF),
            pltpu.VMEM((20, 64, 128), BF),
            pltpu.VMEM((192, 256), BF),
            pltpu.VMEM((3072, 256), BF),
            pltpu.VMEM((2, 256, 128), BF),
            pltpu.VMEM((4608, 256), BF),
            pltpu.VMEM((4608, 256), BF),
            pltpu.VMEM((2, 128, 256), BF),
            pltpu.VMEM((6144, 256), BF),
            pltpu.VMEM((16, 256), F32),
            pltpu.VMEM((18, 368, 256), BF),
            pltpu.VMEM((18, 368, 256), BF),
            pltpu.VMEM((16, 352, 256), BF),
            pltpu.VMEM((3, 8, 176, 256), BF),
            pltpu.VMEM((3, 6, 160, 256), BF),
            pltpu.VMEM((4, 144, 256), BF),
            pltpu.VMEM((2, 2, 6, 128, 256), BF),
            pltpu.VMEM((2, 2, 6, 128, 256), BF),
            pltpu.SemaphoreType.DMA((14,)),
            pltpu.SemaphoreType.DMA((4,)),
            pltpu.SemaphoreType.DMA((4,)),
            pltpu.SemaphoreType.DMA((2,)),
            pltpu.SemaphoreType.DMA((2,)),
            pltpu.SemaphoreType.DMA((2,)),
            pltpu.SemaphoreType.DMA((2,)),
        ],
        compiler_params=pltpu.CompilerParams(
            vmem_limit_bytes=58 * 1024 * 1024, collective_id=0, has_side_effects=True
        ),
    )(*args)
    return d.astype(F32) + jnp.transpose(out, (0, 1, 3, 2))


def solution(mesh):
    placed = (P(None, "gx", "gy", "gz"), P(), P(), P(), P(), P(), P(), P(), P())
    return jax.shard_map(
        local, mesh=mesh, in_specs=placed, out_specs=P(None, "gx", "gy", "gz"), check_vma=False
    )
```

```python
import jax
import jax.numpy as jnp
import numpy as np
from jax import lax
from jax.experimental import pallas as pl
from jax.experimental.pallas import tpu as pltpu
from jax.sharding import PartitionSpec as P

BF = jnp.bfloat16
F32 = jnp.float32


def act(v):
    return jnp.where(v > 0, v, 0.1 * v)


def lift_selection():
    sel = np.zeros((3, 4, 192, 27), np.float32)
    for oy in range(2):
        for oz in range(2):
            for dx in range(3):
                for dy in range(2):
                    for dz in range(2):
                        for jy in range(2):
                            for jz in range(2):
                                b, c = 2 * dy + jy - oy, 2 * dz + jz - oz
                                if 0 <= b < 3 and 0 <= c < 3:
                                    for ch in range(3):
                                        row = (((dx * 2 + dy) * 2 + dz) * 16 + (jy * 2 + jz) * 3 + ch)
                                        sel[ch, oy * 2 + oz, row, 9 * dx + 3 * b + c] = 1
    return sel.reshape(3, 768, 27)


def place_columns():
    place = np.zeros((32, 256), np.float32)
    for jy in range(2):
        for lane in range(128):
            place[2 * (lane // 8) + jy, 128 * jy + lane] = 1
    return place


def gather_rows():
    rows = np.zeros((2, 64, 192), np.float32)
    for jy in range(2):
        for x in range(4):
            for z in range(16):
                for c in range(3):
                    rows[jy, 16 * x + jy * 6 + (z % 2) * 3 + c, 64 * c + 16 * x + z] = 1
    return rows


def spread_head():
    spread = np.zeros((96, 16), np.float32)
    for jy in range(2):
        for k in range(3):
            for z in range(16):
                spread[48 * jy + 16 * k + z, jy * 6 + (z % 2) * 3 + k] = 1
    return spread


def widen_lanes():
    wide = np.zeros((384, 256), np.float32)
    for z in range(8):
        for y in range(16):
            wide[8 * y + z, 16 * y + z + 4] = 1
            wide[128 + 8 * y + z, 16 * y + z % 4] = 1
            wide[256 + 8 * y + z, 16 * y + 12 + z % 4] = 1
    return wide


def dot(a, b):
    return jnp.dot(a, b, preferred_element_type=F32)


def remote(src, dst, send, recv, **where):
    return pltpu.make_async_remote_copy(
        src_ref=src, dst_ref=dst, send_sem=send, recv_sem=recv,
        device_id=where, device_id_type=pl.DeviceIdType.MESH,
    )


def unet(
    disp_hbm, place_hbm, rows_hbm, lw_hbm, sel_hbm, ew_hbm, cw_hbm, wide_hbm,
    m1_hbm, m2_hbm, uw_hbm, dw_hbm, hw_hbm, spr_hbm,
    out,
    disp, place, rows, lw, sel, ew, cw, wide, m1, m2, uw, dw, hw, spr,
    layers, packs, left, right, slab_out, slab_in, sides, whs, mid,
    patch, edge, wl, we, wd, wm1, wm2, wu, wc, wh,
    f0, f1, skip, coarse, middle, deep, ks, ku,
    load_sem, x_send, x_recv, z_send, z_recv, y_send, y_recv,
):
    gx, gy, gz = lax.axis_index("gx"), lax.axis_index("gy"), lax.axis_index("gz")
    nx, ny, nz = lax.axis_size("gx"), lax.axis_size("gy"), lax.axis_size("gz")

    def at_x(step):
        return {"gx": lax.rem(gx + nx + step, nx)}

    def at_y(step):
        return {"gy": lax.rem(gy + ny + step, ny)}

    def at_xz(step, turn):
        return {"gx": lax.rem(gx + nx + step, nx), "gz": lax.rem(gz + nz + turn, nz)}

    steps = (-2, -1, 1, 2)
    barrier = pltpu.get_barrier_semaphore()
    sideways = [(step, turn) for turn in (1, -1) for step in (-2, 2, -1, 1, 0)]
    for where in [at_x(step) for step in steps] + [at_xz(*move) for move in sideways] + [at_y(-1), at_y(1)]:
        pl.semaphore_signal(barrier, inc=1, device_id=where, device_id_type=pl.DeviceIdType.MESH)

    loads = [
        pltpu.make_async_copy(src, dst, load_sem.at[n])
        for n, (src, dst) in enumerate((
            (disp_hbm, disp), (place_hbm, place), (rows_hbm, rows),
            (lw_hbm, lw), (sel_hbm, sel), (ew_hbm, ew), (cw_hbm, cw), (wide_hbm, wide),
            (m1_hbm, m1), (m2_hbm, m2), (uw_hbm, uw), (dw_hbm, dw), (hw_hbm, hw), (spr_hbm, spr),
        ))
    ]
    for load in loads:
        load.start()
    for load in loads[:3]:
        load.wait()

    row_z = lax.broadcasted_iota(jnp.int32, (192, 128), 0) % 16 // 2
    lane_z = lax.broadcasted_iota(jnp.int32, (192, 128), 1) % 8
    keep = row_z == lane_z
    cells = dot(disp[...].reshape(192, 32), place[...])
    own = jnp.zeros((64, 128), F32)
    for jy in range(2):
        part = jnp.where(keep, cells[:, 128 * jy : 128 * jy + 128], 0.0).astype(BF)
        own = own + dot(rows[jy], part)
    layers[8:12] = own.astype(BF).reshape(4, 16, 128)
    first_four = lax.broadcasted_iota(jnp.int32, (2, 16, 128), 2) % 8 < 4
    even, odd = own.reshape(2, 2, 16, 128)[:, 0], own.reshape(2, 2, 16, 128)[:, 1]
    packs[0] = jnp.where(first_four, pltpu.roll(even, 124, axis=2), odd).astype(BF)
    packs[1] = jnp.where(first_four, even, pltpu.roll(odd, 4, axis=2)).astype(BF)

    pl.semaphore_wait(barrier, 16)
    x_copies, z_copies = [], []
    for n, step in enumerate(steps):
        x_copies.append(remote(
            layers.at[8:12], layers.at[pl.ds(8 - 4 * step, 4)], x_send.at[n], x_recv.at[n], **at_x(step)
        ))
    for n, (step, turn) in enumerate(sideways):
        src, dst = (packs.at[0], left) if turn == 1 else (packs.at[1], right)
        z_copies.append(remote(
            src, dst.at[pl.ds(4 - 2 * step, 2)], z_send.at[n], z_recv.at[n], **at_xz(step, turn)
        ))
    for copy in z_copies + x_copies:
        copy.start()

    for load in loads[3:7]:
        load.wait()
    w = dot(sel[0], lw[0]) + dot(sel[1], lw[1]) + dot(sel[2], lw[2])
    w = w.reshape(4, 192, 64)
    wl[:, 0:128] = jnp.concatenate([w[0], w[1]], axis=1).astype(BF)
    wl[:, 128:256] = jnp.concatenate([w[2], w[3]], axis=1).astype(BF)

    def pair_tiles(src, a, b):
        taps = [src[9 * a + 3 * b + c].astype(F32) for c in range(3)]
        none = jnp.zeros_like(taps[0])
        for m in range(4):
            lo = taps[m] if m < 3 else none
            hi = taps[m - 1] if m > 0 else none
            yield m, jnp.transpose(jnp.concatenate([lo, hi], axis=0)).astype(BF)

    we[...] = jnp.zeros_like(we)
    wc[...] = jnp.zeros_like(wc)
    for a in range(3):
        for b in range(3):
            for m, tile in pair_tiles(ew, a, b):
                dz, jz = m // 2, m % 2
                for dy in range(2):
                    for jy in range(2):
                        oy = 2 * dy + jy - b
                        if 0 <= oy < 2:
                            row = ((a * 2 + dy) * 2 + dz) * 256 + (jy * 2 + jz) * 64
                            we[row : row + 64, oy * 128 : oy * 128 + 128] = tile
            for m, tile in pair_tiles(cw, a, b):
                dz, jz = m // 2, m % 2
                for dy in range(2):
                    for jy in range(2):
                        oy = 2 * dy + jy - b
                        if 0 <= oy < 2:
                            for s in range(2):
                                row = (((s * 3 + a) * 2 + dy) * 2 + dz) * 256 + (jy * 2 + jz) * 64
                                wc[row : row + 64, oy * 128 : oy * 128 + 128] = tile[s * 64 : s * 64 + 64]

    for load in loads[7:]:
        load.wait()
    wm1[...] = jnp.zeros_like(wm1)
    wm2[...] = jnp.zeros_like(wm2)
    for a in range(3):
        for b in range(3):
            for c in range(3):
                for src, dst in ((m1, wm1), (m2, wm2)):
                    tile = jnp.transpose(src[9 * a + 3 * b + c].astype(F32)).astype(BF)
                    for dy in range(2):
                        for jy in range(2):
                            oy = 2 * dy + jy - b
                            if 0 <= oy < 2:
                                row = ((a * 2 + dy) * 3 + c) * 256 + jy * 128
                                dst[row : row + 128, oy * 128 : oy * 128 + 128] = tile
    wd[...] = dw[...].reshape(2, 256, 128)
    for a in range(2):
        for b in range(2):
            pairs = jnp.concatenate([uw[4 * a + 2 * b + 1], uw[4 * a + 2 * b]], axis=0).astype(F32)
            wu[a, :, b * 128 : b * 128 + 128] = jnp.transpose(pairs).astype(BF)
    wh[...] = jnp.zeros_like(wh)
    for g in range(4):
        wh[3 * g : 3 * g + 3, 64 * g : 64 * g + 64] = hw[...].astype(F32)
    whs[...] = dot(spr[...], wh[...].astype(BF)).astype(BF)

    for copy in x_copies + z_copies:
        copy.wait_recv()
    first_four = lax.broadcasted_iota(jnp.int32, (10, 16, 128), 2) % 8 < 4
    sides[:, 0:128] = layers[...].reshape(320, 128)
    for n, src in ((1, left), (2, right)):
        pack = src[...].astype(F32)
        split = jnp.stack([jnp.where(first_four, pack, 0.0), jnp.where(first_four, 0.0, pack)], axis=1)
        sides[:, 128 * n : 128 * n + 128] = split.reshape(320, 128).astype(BF)
    mid[...] = dot(sides[...], wide[...]).reshape(20, 16, 256)
    half = lax.broadcasted_iota(jnp.int32, (10, 16, 128), 2) < 64
    pairs = mid[...].reshape(10, 2, 16, 256)
    upper = jnp.where(half, pltpu.roll(pairs[:, 0, :, 128:], 64, axis=2), pairs[:, 1, :, 128:])
    lower = jnp.where(half, pairs[:, 0, :, :128], pltpu.roll(pairs[:, 1, :, :128], 64, axis=2))
    slab_out[0] = upper.astype(BF)
    slab_out[1] = lower.astype(BF)
    y_copies = [
        remote(slab_out.at[0], slab_in.at[0], y_send.at[0], y_recv.at[0], **at_y(1)),
        remote(slab_out.at[1], slab_in.at[1], y_send.at[1], y_recv.at[1], **at_y(-1)),
    ]
    for copy in y_copies:
        copy.start()

    def lay_inner(x):
        q = mid[x]
        for dy in range(2):
            for dz in range(2):
                shift = dy * 16 + dz
                r = pltpu.roll(q, 256 - shift, axis=1) if shift else q
                g = dy * 2 + dz
                patch[x, 16 * g : 16 * g + 16, :] = r.astype(BF)

    lane = lax.broadcasted_iota(jnp.int32, (16, 128), 1)

    def lay_outer(x):
        first, last = mid[x, :, 0:128], mid[x, :, 128:256]
        low, high = slab_in[0, x // 2].astype(F32), slab_in[1, x // 2].astype(F32)
        if x % 2:
            low, high = pltpu.roll(low, 64, axis=1), pltpu.roll(high, 64, axis=1)
        one = jnp.where(lane < 64, low, jnp.where(lane < 80, pltpu.roll(last, 80, axis=1), pltpu.roll(high, 80, axis=1)))
        two = jnp.where(lane < 48, pltpu.roll(low, 112, axis=1), jnp.where(lane < 64, pltpu.roll(first, 48, axis=1), pltpu.roll(high, 64, axis=1)))
        for dy, q in enumerate((one, two)):
            for dz in range(2):
                r = pltpu.roll(q, 127, axis=1) if dz else q
                g = dy * 2 + dz
                edge[x, 16 * g : 16 * g + 16, :] = r.astype(BF)

    def lift(src, x, size):
        p = src[x : x + 3].reshape(192, size)
        v = lax.dot_general(p, wl[...], (((0,), (0,)), ((), ())), preferred_element_type=F32)
        return act(v)

    def lift_inner(x):
        v = lift(patch, x, 256)
        f0[x, 64:304] = v[:240].astype(BF)
        f1[x, 64:304] = pltpu.roll(v, 255, axis=0)[:240].astype(BF)

    def lift_outer(x):
        v = lift(edge, x, 128)
        for dst, r in ((f0, v), (f1, pltpu.roll(v, 127, axis=0))):
            dst[x, 0:64] = r[:64].astype(BF)
            dst[x, 304:368] = r[64:].astype(BF)

    def encode(x, n, spans):
        taps = []
        for a in range(3):
            for dy in range(2):
                for src in (f0, f1):
                    taps.append(jnp.concatenate(
                        [src[x + a + h, r + dy * 16 : r + dy * 16 + size, :] for h in range(n) for r, size in spans], axis=0
                    ))
        v = act(dot(jnp.concatenate(taps, axis=1), we[...])).astype(BF)
        at = 0
        for h in range(n):
            for r, size in spans:
                skip[x + h, r : r + size] = v[at : at + size]
                at += size

    def downward(x):
        lhs = jnp.concatenate([skip[2 * x], skip[2 * x + 1]], axis=1)
        v = act(dot(lhs, wd[...].reshape(512, 128)))
        for c in range(3):
            r = pltpu.roll(v, 352 - c, axis=0) if c else v
            r = r.reshape(11, 2, 16, 128)
            coarse[c, x, :, 0:128] = r[:, 0].reshape(176, 128).astype(BF)
            coarse[c, x, :, 128:256] = r[:, 1].reshape(176, 128).astype(BF)

    def conv_half(src, x, size, weight):
        taps = []
        for a in range(3):
            for dy in range(2):
                for c in range(3):
                    taps.append(src[c, x + a, dy * 16 : dy * 16 + size, :])
        return act(dot(jnp.concatenate(taps, axis=1), weight[...]))

    def conv_first(x):
        v = conv_half(coarse, x, 160, wm1)
        for c in range(3):
            r = pltpu.roll(v, 160 - c, axis=0) if c else v
            middle[c, x] = r.astype(BF)

    def conv_second(x):
        deep[x] = conv_half(middle, x, 144, wm2).astype(BF)

    low = lax.broadcasted_iota(jnp.int32, (17, 16, 128), 2) < 64

    def spread(dst, f, blocks):
        for dz in range(2):
            r = pltpu.roll(blocks, 15, axis=1) if dz else blocks
            r = r[:, 0:8]
            for dy in range(2):
                dst[dy, dz, f] = r[dy : dy + 16].reshape(128, 256).astype(BF)

    def spread_skip(f):
        v = skip[f + 5].astype(F32).reshape(22, 16, 256)
        halves = []
        for jy in range(2):
            s = v[2 + jy : 19 + jy, :, 128 - 128 * jy : 256 - 128 * jy]
            t = jnp.where(low, pltpu.roll(s, 13, axis=1), pltpu.roll(s, 14, axis=1))
            halves.append(pltpu.roll(t, 64, axis=2))
        spread(ks, f, jnp.concatenate(halves, axis=2))

    def upsample(f):
        xd = (f + 1) // 2
        a = (f + 1) % 2
        d = deep[xd]
        us = []
        for jy in range(2):
            us.append(act(dot(d[:, jy * 128 : jy * 128 + 128], wu[a])).reshape(9, 1, 16, 256))
        u = jnp.concatenate(us, axis=1).reshape(18, 16, 256)
        halves = []
        for jy in range(2):
            s = u[jy : 17 + jy, :, 128 - 128 * jy : 256 - 128 * jy]
            halves.append(jnp.where(low, s, pltpu.roll(s, 15, axis=1)))
        spread(ku, f, jnp.concatenate(halves, axis=2))

    def decode(x):
        taps = []
        for src in (ks, ku):
            for a in range(3):
                for dy in range(2):
                    for dz in range(2):
                        taps.append(src[dy, dz, x + a])
        return act(dot(jnp.concatenate(taps, axis=1), wc[...])).astype(BF)

    for x in range(6):
        lay_inner(x)
    for x in range(4):
        lift_inner(x)
    inner, both_ends = ((64, 224),), ((0, 64), (288, 64))
    for x in range(0, 14, 2):
        for h in range(2):
            lay_inner(x + 6 + h)
            lift_inner(x + 4 + h)
        encode(x, 1, inner)
        encode(x + 1, 1, inner)
    for copy in y_copies:
        copy.wait_recv()
    for x in range(10):
        lay_outer(x)
    encode(14, 1, inner)
    for x in range(6):
        lift_outer(x)
    encode(15, 1, inner)
    for x in range(0, 16, 4):
        for h in range(4):
            if x + 10 + h < 20:
                lay_outer(x + 10 + h)
            if x + 6 + h < 18:
                lift_outer(x + 6 + h)
        encode(x, 2, both_ends)
        encode(x + 2, 2, both_ends)
        if x:
            downward(x // 2 - 2)
            downward(x // 2 - 1)
    downward(6)
    spread_skip(0)
    downward(7)
    for x in range(6):
        conv_first(x)
        if x:
            spread_skip(x)
    for x in range(4):
        conv_second(x)
        for f in range(6):
            if (f + 1) // 2 == x - 1:
                upsample(f)
    upsample(5)
    v = jnp.concatenate([decode(x) for x in range(4)], axis=0)

    h = lax.dot_general(whs[...], v, (((1,), (1,)), ((), ())), preferred_element_type=F32)
    spot = lax.broadcasted_iota(jnp.int32, (96, 512), 0) % 16 // 2 == lax.broadcasted_iota(jnp.int32, (96, 512), 1) % 8
    h = jnp.where(spot, h, 0.0)
    rough = h.astype(BF)
    fine = (h - rough.astype(F32)).astype(BF)
    sums = []
    for part in (rough, fine):
        wide_part = jnp.concatenate([
            jnp.concatenate([part[48 * jy : 48 * jy + 48, 128 * x : 128 * x + 128] for x in range(4)], axis=0)
            for jy in range(2)
        ], axis=1)
        sums.append(lax.dot_general(wide_part, place[...], (((1,), (1,)), ((), ())), preferred_element_type=F32))
    total = (sums[0] + sums[1]).reshape(4, 3, 16, 32)
    for x in range(4):
        out[:, x] = total[x]
    for copy in x_copies + z_copies + y_copies:
        copy.wait_send()


def local(d, lw, ew, dw, m1, m2, uw, cw, hw):
    anywhere = pl.BlockSpec(memory_space=pltpu.HBM)
    args = (
        jnp.transpose(d, (0, 1, 3, 2)), jnp.asarray(place_columns(), BF), jnp.asarray(gather_rows(), BF),
        jnp.transpose(lw, (2, 0, 1)), jnp.asarray(lift_selection(), BF), ew, cw, jnp.asarray(widen_lanes(), BF),
        m1, m2, uw, jnp.transpose(dw, (0, 2, 1)), hw, jnp.asarray(spread_head(), BF),
    )
    out = pl.pallas_call(
        unet,
        out_shape=pltpu.VMEM((3, 4, 16, 32), F32),
        in_specs=[anywhere] * 14,
        out_specs=pl.BlockSpec(memory_space=pltpu.VMEM),
        scratch_shapes=[pltpu.VMEM(arg.shape, arg.dtype) for arg in args] + [
            pltpu.VMEM((20, 16, 128), BF),
            pltpu.VMEM((2, 2, 16, 128), BF),
            pltpu.VMEM((10, 16, 128), BF),
            pltpu.VMEM((10, 16, 128), BF),
            pltpu.VMEM((2, 10, 16, 128), BF),
            pltpu.VMEM((2, 10, 16, 128), BF),
            pltpu.VMEM((320, 384), BF),
            pltpu.VMEM((96, 256), BF),
            pltpu.VMEM((20, 16, 256), F32),
            pltpu.VMEM((20, 64, 256), BF),
            pltpu.VMEM((20, 64, 128), BF),
            pltpu.VMEM((192, 256), BF),
            pltpu.VMEM((3072, 256), BF),
            pltpu.VMEM((2, 256, 128), BF),
            pltpu.VMEM((4608, 256), BF),
            pltpu.VMEM((4608, 256), BF),
            pltpu.VMEM((2, 128, 256), BF),
            pltpu.VMEM((6144, 256), BF),
            pltpu.VMEM((16, 256), F32),
            pltpu.VMEM((18, 368, 256), BF),
            pltpu.VMEM((18, 368, 256), BF),
            pltpu.VMEM((16, 352, 256), BF),
            pltpu.VMEM((3, 8, 176, 256), BF),
            pltpu.VMEM((3, 6, 160, 256), BF),
            pltpu.VMEM((4, 144, 256), BF),
            pltpu.VMEM((2, 2, 6, 128, 256), BF),
            pltpu.VMEM((2, 2, 6, 128, 256), BF),
            pltpu.SemaphoreType.DMA((14,)),
            pltpu.SemaphoreType.DMA((4,)),
            pltpu.SemaphoreType.DMA((4,)),
            pltpu.SemaphoreType.DMA((10,)),
            pltpu.SemaphoreType.DMA((10,)),
            pltpu.SemaphoreType.DMA((2,)),
            pltpu.SemaphoreType.DMA((2,)),
        ],
        compiler_params=pltpu.CompilerParams(
            vmem_limit_bytes=58 * 1024 * 1024, collective_id=0, has_side_effects=True
        ),
    )(*args)
    return d.astype(F32) + jnp.transpose(out, (0, 1, 3, 2))


def solution(mesh):
    placed = (P(None, "gx", "gy", "gz"), P(), P(), P(), P(), P(), P(), P(), P())
    return jax.shard_map(
        local, mesh=mesh, in_specs=placed, out_specs=P(None, "gx", "gy", "gz"), check_vma=False
    )
```

```python
import jax
import jax.numpy as jnp
import numpy as np
from jax import lax
from jax.experimental import pallas as pl
from jax.experimental.pallas import tpu as pltpu
from jax.sharding import PartitionSpec as P

BF = jnp.bfloat16
F32 = jnp.float32


def act(v):
    return jnp.where(v > 0, v, 0.1 * v)


def lift_selection():
    sel = np.zeros((3, 4, 192, 27), np.float32)
    for oy in range(2):
        for oz in range(2):
            for dx in range(3):
                for dy in range(2):
                    for dz in range(2):
                        for jy in range(2):
                            for jz in range(2):
                                b, c = 2 * dy + jy - oy, 2 * dz + jz - oz
                                if 0 <= b < 3 and 0 <= c < 3:
                                    for ch in range(3):
                                        row = (((dx * 2 + dy) * 2 + dz) * 16 + (jy * 2 + jz) * 3 + ch)
                                        sel[ch, oy * 2 + oz, row, 9 * dx + 3 * b + c] = 1
    return sel.reshape(3, 768, 27)


def place_columns():
    place = np.zeros((32, 256), np.float32)
    for jy in range(2):
        for lane in range(128):
            place[2 * (lane // 8) + jy, 128 * jy + lane] = 1
    return place


def gather_rows():
    rows = np.zeros((2, 64, 192), np.float32)
    for jy in range(2):
        for x in range(4):
            for z in range(16):
                for c in range(3):
                    rows[jy, 16 * x + jy * 6 + (z % 2) * 3 + c, 64 * c + 16 * x + z] = 1
    return rows


def spread_head():
    spread = np.zeros((96, 16), np.float32)
    for jy in range(2):
        for k in range(3):
            for z in range(16):
                spread[48 * jy + 16 * k + z, jy * 6 + (z % 2) * 3 + k] = 1
    return spread


def widen_lanes():
    wide = np.zeros((384, 256), np.float32)
    for z in range(8):
        for y in range(16):
            wide[8 * y + z, 16 * y + z + 4] = 1
            wide[128 + 8 * y + z, 16 * y + z % 4] = 1
            wide[256 + 8 * y + z, 16 * y + 12 + z % 4] = 1
    return wide


def dot(a, b):
    return jnp.dot(a, b, preferred_element_type=F32)


def remote(src, dst, send, recv, **where):
    return pltpu.make_async_remote_copy(
        src_ref=src, dst_ref=dst, send_sem=send, recv_sem=recv,
        device_id=where, device_id_type=pl.DeviceIdType.MESH,
    )


def unet(
    disp_hbm, place_hbm, rows_hbm, lw_hbm, sel_hbm, ew_hbm, cw_hbm, wide_hbm,
    m1_hbm, m2_hbm, uw_hbm, dw_hbm, hw_hbm, spr_hbm,
    out,
    disp, place, rows, lw, sel, ew, cw, wide, m1, m2, uw, dw, hw, spr,
    layers, packs, left, right, slab_out, slab_in, sides, whs, mid,
    patch, edge, wl, we, wd, wm1, wm2, wu, wc, wh,
    f0, f1, skip, coarse, middle, deep, ks, ku,
    load_sem, x_send, x_recv, z_send, z_recv, y_send, y_recv,
):
    gx, gy, gz = lax.axis_index("gx"), lax.axis_index("gy"), lax.axis_index("gz")
    nx, ny, nz = lax.axis_size("gx"), lax.axis_size("gy"), lax.axis_size("gz")

    def at_x(step):
        return {"gx": lax.rem(gx + nx + step, nx)}

    def at_y(step):
        return {"gy": lax.rem(gy + ny + step, ny)}

    def at_xz(step, turn):
        return {"gx": lax.rem(gx + nx + step, nx), "gz": lax.rem(gz + nz + turn, nz)}

    steps = (-2, -1, 1, 2)
    barrier = pltpu.get_barrier_semaphore()
    sideways = [(step, turn) for turn in (1, -1) for step in (-2, 2, -1, 1, 0)]
    for where in [at_x(step) for step in steps] + [at_xz(*move) for move in sideways] + [at_y(-1), at_y(1)]:
        pl.semaphore_signal(barrier, inc=1, device_id=where, device_id_type=pl.DeviceIdType.MESH)

    loads = [
        pltpu.make_async_copy(src, dst, load_sem.at[n])
        for n, (src, dst) in enumerate((
            (disp_hbm, disp), (place_hbm, place), (rows_hbm, rows),
            (lw_hbm, lw), (sel_hbm, sel), (ew_hbm, ew), (cw_hbm, cw), (wide_hbm, wide),
            (m1_hbm, m1), (m2_hbm, m2), (uw_hbm, uw), (dw_hbm, dw), (hw_hbm, hw), (spr_hbm, spr),
        ))
    ]
    for load in loads[:3]:
        load.start()
    for load in loads[:3]:
        load.wait()
    for load in loads[3:]:
        load.start()

    row_z = lax.broadcasted_iota(jnp.int32, (192, 128), 0) % 16 // 2
    lane_z = lax.broadcasted_iota(jnp.int32, (192, 128), 1) % 8
    keep = row_z == lane_z
    cells = dot(disp[...].reshape(192, 32), place[...])
    own = jnp.zeros((64, 128), F32)
    for jy in range(2):
        part = jnp.where(keep, cells[:, 128 * jy : 128 * jy + 128], 0.0).astype(BF)
        own = own + dot(rows[jy], part)
    layers[8:12] = own.astype(BF).reshape(4, 16, 128)
    first_four = lax.broadcasted_iota(jnp.int32, (2, 16, 128), 2) % 8 < 4
    even, odd = own.reshape(2, 2, 16, 128)[:, 0], own.reshape(2, 2, 16, 128)[:, 1]
    packs[0] = jnp.where(first_four, pltpu.roll(even, 124, axis=2), odd).astype(BF)
    packs[1] = jnp.where(first_four, even, pltpu.roll(odd, 4, axis=2)).astype(BF)

    pl.semaphore_wait(barrier, 16)
    x_copies, z_copies = [], []
    for n, step in enumerate(steps):
        x_copies.append(remote(
            layers.at[8:12], layers.at[pl.ds(8 - 4 * step, 4)], x_send.at[n], x_recv.at[n], **at_x(step)
        ))
    for n, (step, turn) in enumerate(sideways):
        src, dst = (packs.at[0], left) if turn == 1 else (packs.at[1], right)
        z_copies.append(remote(
            src, dst.at[pl.ds(4 - 2 * step, 2)], z_send.at[n], z_recv.at[n], **at_xz(step, turn)
        ))
    for copy in z_copies + x_copies:
        copy.start()

    for load in loads[3:7]:
        load.wait()
    w = dot(sel[0], lw[0]) + dot(sel[1], lw[1]) + dot(sel[2], lw[2])
    w = w.reshape(4, 192, 64)
    wl[:, 0:128] = jnp.concatenate([w[0], w[1]], axis=1).astype(BF)
    wl[:, 128:256] = jnp.concatenate([w[2], w[3]], axis=1).astype(BF)

    def pair_tiles(src, a, b):
        taps = [src[9 * a + 3 * b + c].astype(F32) for c in range(3)]
        none = jnp.zeros_like(taps[0])
        for m in range(4):
            lo = taps[m] if m < 3 else none
            hi = taps[m - 1] if m > 0 else none
            yield m, jnp.transpose(jnp.concatenate([lo, hi], axis=0)).astype(BF)

    we[...] = jnp.zeros_like(we)
    wc[...] = jnp.zeros_like(wc)
    for a in range(3):
        for b in range(3):
            for m, tile in pair_tiles(ew, a, b):
                dz, jz = m // 2, m % 2
                for dy in range(2):
                    for jy in range(2):
                        oy = 2 * dy + jy - b
                        if 0 <= oy < 2:
                            row = ((a * 2 + dy) * 2 + dz) * 256 + (jy * 2 + jz) * 64
                            we[row : row + 64, oy * 128 : oy * 128 + 128] = tile
            for m, tile in pair_tiles(cw, a, b):
                dz, jz = m // 2, m % 2
                for dy in range(2):
                    for jy in range(2):
                        oy = 2 * dy + jy - b
                        if 0 <= oy < 2:
                            for s in range(2):
                                row = (((s * 3 + a) * 2 + dy) * 2 + dz) * 256 + (jy * 2 + jz) * 64
                                wc[row : row + 64, oy * 128 : oy * 128 + 128] = tile[s * 64 : s * 64 + 64]

    for load in loads[7:]:
        load.wait()
    wm1[...] = jnp.zeros_like(wm1)
    wm2[...] = jnp.zeros_like(wm2)
    for a in range(3):
        for b in range(3):
            for c in range(3):
                for src, dst in ((m1, wm1), (m2, wm2)):
                    tile = jnp.transpose(src[9 * a + 3 * b + c].astype(F32)).astype(BF)
                    for dy in range(2):
                        for jy in range(2):
                            oy = 2 * dy + jy - b
                            if 0 <= oy < 2:
                                row = ((a * 2 + dy) * 3 + c) * 256 + jy * 128
                                dst[row : row + 128, oy * 128 : oy * 128 + 128] = tile
    wd[...] = dw[...].reshape(2, 256, 128)
    for a in range(2):
        for b in range(2):
            pairs = jnp.concatenate([uw[4 * a + 2 * b + 1], uw[4 * a + 2 * b]], axis=0).astype(F32)
            wu[a, :, b * 128 : b * 128 + 128] = jnp.transpose(pairs).astype(BF)
    wh[...] = jnp.zeros_like(wh)
    for g in range(4):
        wh[3 * g : 3 * g + 3, 64 * g : 64 * g + 64] = hw[...].astype(F32)
    whs[...] = dot(spr[...], wh[...].astype(BF)).astype(BF)

    for copy in x_copies + z_copies:
        copy.wait_recv()
    first_four = lax.broadcasted_iota(jnp.int32, (10, 16, 128), 2) % 8 < 4
    sides[:, 0:128] = layers[...].reshape(320, 128)
    for n, src in ((1, left), (2, right)):
        pack = src[...].astype(F32)
        split = jnp.stack([jnp.where(first_four, pack, 0.0), jnp.where(first_four, 0.0, pack)], axis=1)
        sides[:, 128 * n : 128 * n + 128] = split.reshape(320, 128).astype(BF)
    for n in range(2):
        mid[10 * n : 10 * n + 10] = dot(sides[160 * n : 160 * n + 160], wide[...]).reshape(10, 16, 256)
    def lay_inner(x):
        q = mid[x]
        for dy in range(2):
            for dz in range(2):
                shift = dy * 16 + dz
                r = pltpu.roll(q, 256 - shift, axis=1) if shift else q
                g = dy * 2 + dz
                patch[x, 16 * g : 16 * g + 16, :] = r.astype(BF)

    lane = lax.broadcasted_iota(jnp.int32, (16, 128), 1)

    def lay_outer(x):
        first, last = mid[x, :, 0:128], mid[x, :, 128:256]
        low, high = slab_in[0, x // 2].astype(F32), slab_in[1, x // 2].astype(F32)
        if x % 2:
            low, high = pltpu.roll(low, 64, axis=1), pltpu.roll(high, 64, axis=1)
        one = jnp.where(lane < 64, low, jnp.where(lane < 80, pltpu.roll(last, 80, axis=1), pltpu.roll(high, 80, axis=1)))
        two = jnp.where(lane < 48, pltpu.roll(low, 112, axis=1), jnp.where(lane < 64, pltpu.roll(first, 48, axis=1), pltpu.roll(high, 64, axis=1)))
        for dy, q in enumerate((one, two)):
            for dz in range(2):
                r = pltpu.roll(q, 127, axis=1) if dz else q
                g = dy * 2 + dz
                edge[x, 16 * g : 16 * g + 16, :] = r.astype(BF)

    def lift(src, x, size):
        p = src[x : x + 3].reshape(192, size)
        v = lax.dot_general(p, wl[...], (((0,), (0,)), ((), ())), preferred_element_type=F32)
        return act(v)

    def lift_inner(x):
        v = lift(patch, x, 256)
        f0[x, 64:304] = v[:240].astype(BF)
        f1[x, 64:304] = pltpu.roll(v, 255, axis=0)[:240].astype(BF)

    def lift_outer(x):
        v = lift(edge, x, 128)
        for dst, r in ((f0, v), (f1, pltpu.roll(v, 127, axis=0))):
            dst[x, 0:64] = r[:64].astype(BF)
            dst[x, 304:368] = r[64:].astype(BF)

    def encode(x, n, spans):
        taps = []
        for a in range(3):
            for dy in range(2):
                for src in (f0, f1):
                    taps.append(jnp.concatenate(
                        [src[x + a + h, r + dy * 16 : r + dy * 16 + size, :] for h in range(n) for r, size in spans], axis=0
                    ))
        v = act(dot(jnp.concatenate(taps, axis=1), we[...])).astype(BF)
        at = 0
        for h in range(n):
            for r, size in spans:
                skip[x + h, r : r + size] = v[at : at + size]
                at += size

    def downward(x):
        lhs = jnp.concatenate([skip[2 * x], skip[2 * x + 1]], axis=1)
        v = act(dot(lhs, wd[...].reshape(512, 128)))
        for c in range(3):
            r = pltpu.roll(v, 352 - c, axis=0) if c else v
            r = r.reshape(11, 2, 16, 128)
            coarse[c, x, :, 0:128] = r[:, 0].reshape(176, 128).astype(BF)
            coarse[c, x, :, 128:256] = r[:, 1].reshape(176, 128).astype(BF)

    def conv_half(src, x, size, weight):
        taps = []
        for a in range(3):
            for dy in range(2):
                for c in range(3):
                    taps.append(src[c, x + a, dy * 16 : dy * 16 + size, :])
        return act(dot(jnp.concatenate(taps, axis=1), weight[...]))

    def conv_first(x):
        v = conv_half(coarse, x, 160, wm1)
        for c in range(3):
            r = pltpu.roll(v, 160 - c, axis=0) if c else v
            middle[c, x] = r.astype(BF)

    def conv_second(x):
        deep[x] = conv_half(middle, x, 144, wm2).astype(BF)

    low = lax.broadcasted_iota(jnp.int32, (17, 16, 128), 2) < 64

    def spread(dst, f, blocks):
        for dz in range(2):
            r = pltpu.roll(blocks, 15, axis=1) if dz else blocks
            r = r[:, 0:8]
            for dy in range(2):
                dst[dy, dz, f] = r[dy : dy + 16].reshape(128, 256).astype(BF)

    def spread_skip(f):
        v = skip[f + 5].astype(F32).reshape(22, 16, 256)
        halves = []
        for jy in range(2):
            s = v[2 + jy : 19 + jy, :, 128 - 128 * jy : 256 - 128 * jy]
            t = jnp.where(low, pltpu.roll(s, 13, axis=1), pltpu.roll(s, 14, axis=1))
            halves.append(pltpu.roll(t, 64, axis=2))
        spread(ks, f, jnp.concatenate(halves, axis=2))

    def upsample(f):
        xd = (f + 1) // 2
        a = (f + 1) % 2
        d = deep[xd]
        us = []
        for jy in range(2):
            us.append(act(dot(d[:, jy * 128 : jy * 128 + 128], wu[a])).reshape(9, 1, 16, 256))
        u = jnp.concatenate(us, axis=1).reshape(18, 16, 256)
        halves = []
        for jy in range(2):
            s = u[jy : 17 + jy, :, 128 - 128 * jy : 256 - 128 * jy]
            halves.append(jnp.where(low, s, pltpu.roll(s, 15, axis=1)))
        spread(ku, f, jnp.concatenate(halves, axis=2))

    def decode(x):
        taps = []
        for src in (ks, ku):
            for a in range(3):
                for dy in range(2):
                    for dz in range(2):
                        taps.append(src[dy, dz, x + a])
        return act(dot(jnp.concatenate(taps, axis=1), wc[...])).astype(BF)

    for x in range(6):
        lay_inner(x)
    for x in range(4):
        lift_inner(x)
    half = lax.broadcasted_iota(jnp.int32, (10, 16, 128), 2) < 64
    pairs = mid[...].reshape(10, 2, 16, 256)
    upper = jnp.where(half, pltpu.roll(pairs[:, 0, :, 128:], 64, axis=2), pairs[:, 1, :, 128:])
    lower = jnp.where(half, pairs[:, 0, :, :128], pltpu.roll(pairs[:, 1, :, :128], 64, axis=2))
    slab_out[0] = upper.astype(BF)
    slab_out[1] = lower.astype(BF)
    y_copies = [
        remote(slab_out.at[0], slab_in.at[0], y_send.at[0], y_recv.at[0], **at_y(1)),
        remote(slab_out.at[1], slab_in.at[1], y_send.at[1], y_recv.at[1], **at_y(-1)),
    ]
    for copy in y_copies:
        copy.start()

    inner, both_ends = ((64, 224),), ((0, 64), (288, 64))
    for x in range(0, 12, 2):
        for h in range(2):
            lay_inner(x + 6 + h)
            lift_inner(x + 4 + h)
        encode(x, 1, inner)
        encode(x + 1, 1, inner)
    for copy in y_copies:
        copy.wait_recv()
    for x in range(18, 20):
        lay_inner(x)
    for x in range(16, 18):
        lift_inner(x)
    encode(12, 1, inner)
    for x in range(10):
        lay_outer(x)
    encode(13, 1, inner)
    encode(14, 1, inner)
    for x in range(6):
        lift_outer(x)
    encode(15, 1, inner)
    for x in range(0, 16, 4):
        for h in range(4):
            if x + 10 + h < 20:
                lay_outer(x + 10 + h)
            if x + 6 + h < 18:
                lift_outer(x + 6 + h)
        encode(x, 2, both_ends)
        encode(x + 2, 2, both_ends)
        if x:
            downward(x // 2 - 2)
            downward(x // 2 - 1)
    downward(6)
    spread_skip(0)
    downward(7)
    for x in range(6):
        conv_first(x)
        if x:
            spread_skip(x)
    for x in range(4):
        conv_second(x)
        for f in range(6):
            if (f + 1) // 2 == x - 1:
                upsample(f)
    upsample(5)
    v = jnp.concatenate([decode(x) for x in range(4)], axis=0)

    h = lax.dot_general(whs[...], v, (((1,), (1,)), ((), ())), preferred_element_type=F32)
    spot = lax.broadcasted_iota(jnp.int32, (96, 512), 0) % 16 // 2 == lax.broadcasted_iota(jnp.int32, (96, 512), 1) % 8
    h = jnp.where(spot, h, 0.0)
    rough = h.astype(BF)
    fine = (h - rough.astype(F32)).astype(BF)
    sums = []
    for part in (rough, fine):
        wide_part = jnp.concatenate([
            jnp.concatenate([part[48 * jy : 48 * jy + 48, 128 * x : 128 * x + 128] for x in range(4)], axis=0)
            for jy in range(2)
        ], axis=1)
        sums.append(lax.dot_general(wide_part, place[...], (((1,), (1,)), ((), ())), preferred_element_type=F32))
    total = (sums[0] + sums[1]).reshape(4, 3, 16, 32)
    for x in range(4):
        out[:, x] = total[x]
    for copy in x_copies + z_copies + y_copies:
        copy.wait_send()


def local(d, lw, ew, dw, m1, m2, uw, cw, hw):
    anywhere = pl.BlockSpec(memory_space=pltpu.HBM)
    args = (
        jnp.transpose(d, (0, 1, 3, 2)), jnp.asarray(place_columns(), BF), jnp.asarray(gather_rows(), BF),
        jnp.transpose(lw, (2, 0, 1)), jnp.asarray(lift_selection(), BF), ew, cw, jnp.asarray(widen_lanes(), BF),
        m1, m2, uw, jnp.transpose(dw, (0, 2, 1)), hw, jnp.asarray(spread_head(), BF),
    )
    out = pl.pallas_call(
        unet,
        out_shape=pltpu.VMEM((3, 4, 16, 32), F32),
        in_specs=[anywhere] * 14,
        out_specs=pl.BlockSpec(memory_space=pltpu.VMEM),
        scratch_shapes=[pltpu.VMEM(arg.shape, arg.dtype) for arg in args] + [
            pltpu.VMEM((20, 16, 128), BF),
            pltpu.VMEM((2, 2, 16, 128), BF),
            pltpu.VMEM((10, 16, 128), BF),
            pltpu.VMEM((10, 16, 128), BF),
            pltpu.VMEM((2, 10, 16, 128), BF),
            pltpu.VMEM((2, 10, 16, 128), BF),
            pltpu.VMEM((320, 384), BF),
            pltpu.VMEM((96, 256), BF),
            pltpu.VMEM((20, 16, 256), F32),
            pltpu.VMEM((20, 64, 256), BF),
            pltpu.VMEM((20, 64, 128), BF),
            pltpu.VMEM((192, 256), BF),
            pltpu.VMEM((3072, 256), BF),
            pltpu.VMEM((2, 256, 128), BF),
            pltpu.VMEM((4608, 256), BF),
            pltpu.VMEM((4608, 256), BF),
            pltpu.VMEM((2, 128, 256), BF),
            pltpu.VMEM((6144, 256), BF),
            pltpu.VMEM((16, 256), F32),
            pltpu.VMEM((18, 368, 256), BF),
            pltpu.VMEM((18, 368, 256), BF),
            pltpu.VMEM((16, 352, 256), BF),
            pltpu.VMEM((3, 8, 176, 256), BF),
            pltpu.VMEM((3, 6, 160, 256), BF),
            pltpu.VMEM((4, 144, 256), BF),
            pltpu.VMEM((2, 2, 6, 128, 256), BF),
            pltpu.VMEM((2, 2, 6, 128, 256), BF),
            pltpu.SemaphoreType.DMA((14,)),
            pltpu.SemaphoreType.DMA((4,)),
            pltpu.SemaphoreType.DMA((4,)),
            pltpu.SemaphoreType.DMA((10,)),
            pltpu.SemaphoreType.DMA((10,)),
            pltpu.SemaphoreType.DMA((2,)),
            pltpu.SemaphoreType.DMA((2,)),
        ],
        compiler_params=pltpu.CompilerParams(
            vmem_limit_bytes=58 * 1024 * 1024, collective_id=0, has_side_effects=True
        ),
    )(*args)
    return d.astype(F32) + jnp.transpose(out, (0, 1, 3, 2))


def solution(mesh):
    placed = (P(None, "gx", "gy", "gz"), P(), P(), P(), P(), P(), P(), P(), P())
    return jax.shard_map(
        local, mesh=mesh, in_specs=placed, out_specs=P(None, "gx", "gy", "gz"), check_vma=False
    )
```

```python
import jax
import jax.numpy as jnp
import numpy as np
from jax import lax
from jax.experimental import pallas as pl
from jax.experimental.pallas import tpu as pltpu
from jax.sharding import PartitionSpec as P

BF = jnp.bfloat16
F32 = jnp.float32


def act(v):
    return jnp.where(v > 0, v, 0.1 * v)


def lift_selection():
    sel = np.zeros((3, 4, 192, 27), np.float32)
    for oy in range(2):
        for oz in range(2):
            for dx in range(3):
                for dy in range(2):
                    for dz in range(2):
                        for jy in range(2):
                            for jz in range(2):
                                b, c = 2 * dy + jy - oy, 2 * dz + jz - oz
                                if 0 <= b < 3 and 0 <= c < 3:
                                    for ch in range(3):
                                        row = (((dx * 2 + dy) * 2 + dz) * 16 + (jy * 2 + jz) * 3 + ch)
                                        sel[ch, oy * 2 + oz, row, 9 * dx + 3 * b + c] = 1
    return sel.reshape(3, 768, 27)


def place_columns():
    place = np.zeros((32, 256), np.float32)
    for jy in range(2):
        for lane in range(128):
            place[2 * (lane // 8) + jy, 128 * jy + lane] = 1
    return place


def gather_rows():
    rows = np.zeros((2, 64, 192), np.float32)
    for jy in range(2):
        for x in range(4):
            for z in range(16):
                for c in range(3):
                    rows[jy, 16 * x + jy * 6 + (z % 2) * 3 + c, 64 * c + 16 * x + z] = 1
    return rows


def spread_head():
    spread = np.zeros((96, 16), np.float32)
    for jy in range(2):
        for k in range(3):
            for z in range(16):
                spread[48 * jy + 16 * k + z, jy * 6 + (z % 2) * 3 + k] = 1
    return spread


def widen_lanes():
    wide = np.zeros((384, 256), np.float32)
    for z in range(8):
        for y in range(16):
            wide[8 * y + z, 16 * y + z + 4] = 1
            wide[128 + 8 * y + z, 16 * y + z % 4] = 1
            wide[256 + 8 * y + z, 16 * y + 12 + z % 4] = 1
    return wide


def dot(a, b):
    return jnp.dot(a, b, preferred_element_type=F32)


def remote(src, dst, send, recv, **where):
    return pltpu.make_async_remote_copy(
        src_ref=src, dst_ref=dst, send_sem=send, recv_sem=recv,
        device_id=where, device_id_type=pl.DeviceIdType.MESH,
    )


def unet(
    disp_hbm, place_hbm, rows_hbm, lw_hbm, sel_hbm, ew_hbm, cw_hbm, wide_hbm,
    m1_hbm, m2_hbm, uw_hbm, dw_hbm, hw_hbm, spr_hbm,
    out,
    disp, place, rows, lw, sel, ew, cw, wide, m1, m2, uw, dw, hw, spr,
    layers, packs, left, right, slab_out, slab_in, sides, whs, mid,
    patch, edge, wl, we, wd, wm1, wm2, wu, wc, wh,
    f0, f1, skip, coarse, middle, deep, ks, ku,
    load_sem, x_send, x_recv, z_send, z_recv, y_send, y_recv,
):
    gx, gy, gz = lax.axis_index("gx"), lax.axis_index("gy"), lax.axis_index("gz")
    nx, ny, nz = lax.axis_size("gx"), lax.axis_size("gy"), lax.axis_size("gz")

    def at_x(step):
        return {"gx": lax.rem(gx + nx + step, nx)}

    def at_y(step):
        return {"gy": lax.rem(gy + ny + step, ny)}

    def at_xz(step, turn):
        return {"gx": lax.rem(gx + nx + step, nx), "gz": lax.rem(gz + nz + turn, nz)}

    steps = (-2, -1, 1, 2)
    barrier = pltpu.get_barrier_semaphore()
    sideways = [(step, turn) for turn in (1, -1) for step in (-2, 2, -1, 1, 0)]
    for where in [at_x(step) for step in steps] + [at_xz(*move) for move in sideways] + [at_y(-1), at_y(1)]:
        pl.semaphore_signal(barrier, inc=1, device_id=where, device_id_type=pl.DeviceIdType.MESH)

    loads = [
        pltpu.make_async_copy(src, dst, load_sem.at[n])
        for n, (src, dst) in enumerate((
            (disp_hbm, disp), (place_hbm, place), (rows_hbm, rows),
            (lw_hbm, lw), (sel_hbm, sel), (ew_hbm, ew), (cw_hbm, cw), (wide_hbm, wide),
            (m1_hbm, m1), (m2_hbm, m2), (uw_hbm, uw), (dw_hbm, dw), (hw_hbm, hw), (spr_hbm, spr),
        ))
    ]
    for load in loads[:3]:
        load.start()
    for load in loads[:3]:
        load.wait()
    for load in loads[3:]:
        load.start()

    row_z = lax.broadcasted_iota(jnp.int32, (192, 128), 0) % 16 // 2
    lane_z = lax.broadcasted_iota(jnp.int32, (192, 128), 1) % 8
    keep = row_z == lane_z
    cells = dot(disp[...].reshape(192, 32), place[...])
    own = jnp.zeros((64, 128), F32)
    for jy in range(2):
        part = jnp.where(keep, cells[:, 128 * jy : 128 * jy + 128], 0.0).astype(BF)
        own = own + dot(rows[jy], part)
    layers[8:12] = own.astype(BF).reshape(4, 16, 128)
    first_four = lax.broadcasted_iota(jnp.int32, (2, 16, 128), 2) % 8 < 4
    even, odd = own.reshape(2, 2, 16, 128)[:, 0], own.reshape(2, 2, 16, 128)[:, 1]
    packs[0] = jnp.where(first_four, pltpu.roll(even, 124, axis=2), odd).astype(BF)
    packs[1] = jnp.where(first_four, even, pltpu.roll(odd, 4, axis=2)).astype(BF)

    pl.semaphore_wait(barrier, 16)
    x_copies, z_copies = [], []
    for n, step in enumerate(steps):
        x_copies.append(remote(
            layers.at[8:12], layers.at[pl.ds(8 - 4 * step, 4)], x_send.at[n], x_recv.at[n], **at_x(step)
        ))
    for n, (step, turn) in enumerate(sideways):
        src, dst = (packs.at[0], left) if turn == 1 else (packs.at[1], right)
        z_copies.append(remote(
            src, dst.at[pl.ds(4 - 2 * step, 2)], z_send.at[n], z_recv.at[n], **at_xz(step, turn)
        ))
    far, near = [x_copies[0], x_copies[3]], x_copies[1:3]
    for copy in far + z_copies[0:2] + z_copies[5:7] + near + z_copies[2:5] + z_copies[7:10]:
        copy.start()

    for load in loads[3:7]:
        load.wait()
    w = dot(sel[0], lw[0]) + dot(sel[1], lw[1]) + dot(sel[2], lw[2])
    w = w.reshape(4, 192, 64)
    wl[:, 0:128] = jnp.concatenate([w[0], w[1]], axis=1).astype(BF)
    wl[:, 128:256] = jnp.concatenate([w[2], w[3]], axis=1).astype(BF)

    def pair_tiles(src, a, b):
        taps = [src[9 * a + 3 * b + c].astype(F32) for c in range(3)]
        none = jnp.zeros_like(taps[0])
        for m in range(4):
            lo = taps[m] if m < 3 else none
            hi = taps[m - 1] if m > 0 else none
            yield m, jnp.transpose(jnp.concatenate([lo, hi], axis=0)).astype(BF)

    we[...] = jnp.zeros_like(we)
    wc[...] = jnp.zeros_like(wc)
    for a in range(3):
        for b in range(3):
            for m, tile in pair_tiles(ew, a, b):
                dz, jz = m // 2, m % 2
                for dy in range(2):
                    for jy in range(2):
                        oy = 2 * dy + jy - b
                        if 0 <= oy < 2:
                            row = ((a * 2 + dy) * 2 + dz) * 256 + (jy * 2 + jz) * 64
                            we[row : row + 64, oy * 128 : oy * 128 + 128] = tile
            for m, tile in pair_tiles(cw, a, b):
                dz, jz = m // 2, m % 2
                for dy in range(2):
                    for jy in range(2):
                        oy = 2 * dy + jy - b
                        if 0 <= oy < 2:
                            for s in range(2):
                                row = (((s * 3 + a) * 2 + dy) * 2 + dz) * 256 + (jy * 2 + jz) * 64
                                wc[row : row + 64, oy * 128 : oy * 128 + 128] = tile[s * 64 : s * 64 + 64]

    for load in loads[7:]:
        load.wait()
    wm1[...] = jnp.zeros_like(wm1)
    wm2[...] = jnp.zeros_like(wm2)
    for a in range(3):
        for b in range(3):
            for c in range(3):
                for src, dst in ((m1, wm1), (m2, wm2)):
                    tile = jnp.transpose(src[9 * a + 3 * b + c].astype(F32)).astype(BF)
                    for dy in range(2):
                        for jy in range(2):
                            oy = 2 * dy + jy - b
                            if 0 <= oy < 2:
                                row = ((a * 2 + dy) * 3 + c) * 256 + jy * 128
                                dst[row : row + 128, oy * 128 : oy * 128 + 128] = tile
    wd[...] = dw[...].reshape(2, 256, 128)
    for a in range(2):
        for b in range(2):
            pairs = jnp.concatenate([uw[4 * a + 2 * b + 1], uw[4 * a + 2 * b]], axis=0).astype(F32)
            wu[a, :, b * 128 : b * 128 + 128] = jnp.transpose(pairs).astype(BF)
    wh[...] = jnp.zeros_like(wh)
    for g in range(4):
        wh[3 * g : 3 * g + 3, 64 * g : 64 * g + 64] = hw[...].astype(F32)
    whs[...] = dot(spr[...], wh[...].astype(BF)).astype(BF)

    for copy in x_copies + z_copies:
        copy.wait_recv()
    first_four = lax.broadcasted_iota(jnp.int32, (10, 16, 128), 2) % 8 < 4
    sides[:, 0:128] = layers[...].reshape(320, 128)
    for n, src in ((1, left), (2, right)):
        pack = src[...].astype(F32)
        split = jnp.stack([jnp.where(first_four, pack, 0.0), jnp.where(first_four, 0.0, pack)], axis=1)
        sides[:, 128 * n : 128 * n + 128] = split.reshape(320, 128).astype(BF)
    for n in range(2):
        mid[10 * n : 10 * n + 10] = dot(sides[160 * n : 160 * n + 160], wide[...]).reshape(10, 16, 256)
    def lay_inner(x):
        q = mid[x]
        for dy in range(2):
            for dz in range(2):
                shift = dy * 16 + dz
                r = pltpu.roll(q, 256 - shift, axis=1) if shift else q
                g = dy * 2 + dz
                patch[x, 16 * g : 16 * g + 16, :] = r.astype(BF)

    lane = lax.broadcasted_iota(jnp.int32, (16, 128), 1)

    def lay_outer(x):
        first, last = mid[x, :, 0:128], mid[x, :, 128:256]
        low, high = slab_in[0, x // 2].astype(F32), slab_in[1, x // 2].astype(F32)
        if x % 2:
            low, high = pltpu.roll(low, 64, axis=1), pltpu.roll(high, 64, axis=1)
        one = jnp.where(lane < 64, low, jnp.where(lane < 80, pltpu.roll(last, 80, axis=1), pltpu.roll(high, 80, axis=1)))
        two = jnp.where(lane < 48, pltpu.roll(low, 112, axis=1), jnp.where(lane < 64, pltpu.roll(first, 48, axis=1), pltpu.roll(high, 64, axis=1)))
        for dy, q in enumerate((one, two)):
            for dz in range(2):
                r = pltpu.roll(q, 127, axis=1) if dz else q
                g = dy * 2 + dz
                edge[x, 16 * g : 16 * g + 16, :] = r.astype(BF)

    def lift(src, x, size):
        p = src[x : x + 3].reshape(192, size)
        v = lax.dot_general(p, wl[...], (((0,), (0,)), ((), ())), preferred_element_type=F32)
        return act(v)

    def lift_inner(x):
        v = lift(patch, x, 256)
        f0[x, 64:304] = v[:240].astype(BF)
        f1[x, 64:304] = pltpu.roll(v, 255, axis=0)[:240].astype(BF)

    def lift_outer(x):
        v = lift(edge, x, 128)
        for dst, r in ((f0, v), (f1, pltpu.roll(v, 127, axis=0))):
            dst[x, 0:64] = r[:64].astype(BF)
            dst[x, 304:368] = r[64:].astype(BF)

    def encode(x, n, spans):
        taps = []
        for a in range(3):
            for dy in range(2):
                for src in (f0, f1):
                    taps.append(jnp.concatenate(
                        [src[x + a + h, r + dy * 16 : r + dy * 16 + size, :] for h in range(n) for r, size in spans], axis=0
                    ))
        v = act(dot(jnp.concatenate(taps, axis=1), we[...])).astype(BF)
        at = 0
        for h in range(n):
            for r, size in spans:
                skip[x + h, r : r + size] = v[at : at + size]
                at += size

    def downward(x):
        lhs = jnp.concatenate([skip[2 * x], skip[2 * x + 1]], axis=1)
        v = act(dot(lhs, wd[...].reshape(512, 128)))
        for c in range(3):
            r = pltpu.roll(v, 352 - c, axis=0) if c else v
            r = r.reshape(11, 2, 16, 128)
            coarse[c, x, :, 0:128] = r[:, 0].reshape(176, 128).astype(BF)
            coarse[c, x, :, 128:256] = r[:, 1].reshape(176, 128).astype(BF)

    def conv_half(src, x, size, weight):
        taps = []
        for a in range(3):
            for dy in range(2):
                for c in range(3):
                    taps.append(src[c, x + a, dy * 16 : dy * 16 + size, :])
        return act(dot(jnp.concatenate(taps, axis=1), weight[...]))

    def conv_first(x):
        v = conv_half(coarse, x, 160, wm1)
        for c in range(3):
            r = pltpu.roll(v, 160 - c, axis=0) if c else v
            middle[c, x] = r.astype(BF)

    def conv_second(x):
        deep[x] = conv_half(middle, x, 144, wm2).astype(BF)

    low = lax.broadcasted_iota(jnp.int32, (17, 16, 128), 2) < 64

    def spread(dst, f, blocks):
        for dz in range(2):
            r = pltpu.roll(blocks, 15, axis=1) if dz else blocks
            r = r[:, 0:8]
            for dy in range(2):
                dst[dy, dz, f] = r[dy : dy + 16].reshape(128, 256).astype(BF)

    def spread_skip(f):
        v = skip[f + 5].astype(F32).reshape(22, 16, 256)
        halves = []
        for jy in range(2):
            s = v[2 + jy : 19 + jy, :, 128 - 128 * jy : 256 - 128 * jy]
            t = jnp.where(low, pltpu.roll(s, 13, axis=1), pltpu.roll(s, 14, axis=1))
            halves.append(pltpu.roll(t, 64, axis=2))
        spread(ks, f, jnp.concatenate(halves, axis=2))

    def upsample(f):
        xd = (f + 1) // 2
        a = (f + 1) % 2
        d = deep[xd]
        us = []
        for jy in range(2):
            us.append(act(dot(d[:, jy * 128 : jy * 128 + 128], wu[a])).reshape(9, 1, 16, 256))
        u = jnp.concatenate(us, axis=1).reshape(18, 16, 256)
        halves = []
        for jy in range(2):
            s = u[jy : 17 + jy, :, 128 - 128 * jy : 256 - 128 * jy]
            halves.append(jnp.where(low, s, pltpu.roll(s, 15, axis=1)))
        spread(ku, f, jnp.concatenate(halves, axis=2))

    def decode(x):
        taps = []
        for src in (ks, ku):
            for a in range(3):
                for dy in range(2):
                    for dz in range(2):
                        taps.append(src[dy, dz, x + a])
        return act(dot(jnp.concatenate(taps, axis=1), wc[...])).astype(BF)

    for x in range(6):
        lay_inner(x)
    for x in range(4):
        lift_inner(x)
    half = lax.broadcasted_iota(jnp.int32, (10, 16, 128), 2) < 64
    pairs = mid[...].reshape(10, 2, 16, 256)
    upper = jnp.where(half, pltpu.roll(pairs[:, 0, :, 128:], 64, axis=2), pairs[:, 1, :, 128:])
    lower = jnp.where(half, pairs[:, 0, :, :128], pltpu.roll(pairs[:, 1, :, :128], 64, axis=2))
    slab_out[0] = upper.astype(BF)
    slab_out[1] = lower.astype(BF)
    y_copies = [
        remote(slab_out.at[0], slab_in.at[0], y_send.at[0], y_recv.at[0], **at_y(1)),
        remote(slab_out.at[1], slab_in.at[1], y_send.at[1], y_recv.at[1], **at_y(-1)),
    ]
    for copy in y_copies:
        copy.start()

    inner, both_ends = ((64, 224),), ((0, 64), (288, 64))
    for x in range(0, 12, 2):
        for h in range(2):
            lay_inner(x + 6 + h)
            lift_inner(x + 4 + h)
        encode(x, 1, inner)
        encode(x + 1, 1, inner)
    for copy in y_copies:
        copy.wait_recv()
    for x in range(18, 20):
        lay_inner(x)
    for x in range(16, 18):
        lift_inner(x)
    encode(12, 1, inner)
    for x in range(10):
        lay_outer(x)
    encode(13, 1, inner)
    encode(14, 1, inner)
    for x in range(6):
        lift_outer(x)
    encode(15, 1, inner)
    for x in range(0, 16, 4):
        for h in range(4):
            if x + 10 + h < 20:
                lay_outer(x + 10 + h)
            if x + 6 + h < 18:
                lift_outer(x + 6 + h)
        encode(x, 2, both_ends)
        encode(x + 2, 2, both_ends)
        if x:
            downward(x // 2 - 2)
            downward(x // 2 - 1)
    downward(6)
    spread_skip(0)
    downward(7)
    for x in range(6):
        conv_first(x)
        if x:
            spread_skip(x)
    for x in range(4):
        conv_second(x)
        for f in range(6):
            if (f + 1) // 2 == x - 1:
                upsample(f)
    upsample(5)
    v = jnp.concatenate([decode(x) for x in range(4)], axis=0)

    h = lax.dot_general(whs[...], v, (((1,), (1,)), ((), ())), preferred_element_type=F32)
    spot = lax.broadcasted_iota(jnp.int32, (96, 512), 0) % 16 // 2 == lax.broadcasted_iota(jnp.int32, (96, 512), 1) % 8
    h = jnp.where(spot, h, 0.0)
    rough = h.astype(BF)
    fine = (h - rough.astype(F32)).astype(BF)
    sums = []
    for part in (rough, fine):
        wide_part = jnp.concatenate([
            jnp.concatenate([part[48 * jy : 48 * jy + 48, 128 * x : 128 * x + 128] for x in range(4)], axis=0)
            for jy in range(2)
        ], axis=1)
        sums.append(lax.dot_general(wide_part, place[...], (((1,), (1,)), ((), ())), preferred_element_type=F32))
    total = (sums[0] + sums[1]).reshape(4, 3, 16, 32)
    for x in range(4):
        out[:, x] = total[x]
    for copy in x_copies + z_copies + y_copies:
        copy.wait_send()


def local(d, lw, ew, dw, m1, m2, uw, cw, hw):
    anywhere = pl.BlockSpec(memory_space=pltpu.HBM)
    args = (
        jnp.transpose(d, (0, 1, 3, 2)), jnp.asarray(place_columns(), BF), jnp.asarray(gather_rows(), BF),
        jnp.transpose(lw, (2, 0, 1)), jnp.asarray(lift_selection(), BF), ew, cw, jnp.asarray(widen_lanes(), BF),
        m1, m2, uw, jnp.transpose(dw, (0, 2, 1)), hw, jnp.asarray(spread_head(), BF),
    )
    out = pl.pallas_call(
        unet,
        out_shape=pltpu.VMEM((3, 4, 16, 32), F32),
        in_specs=[anywhere] * 14,
        out_specs=pl.BlockSpec(memory_space=pltpu.VMEM),
        scratch_shapes=[pltpu.VMEM(arg.shape, arg.dtype) for arg in args] + [
            pltpu.VMEM((20, 16, 128), BF),
            pltpu.VMEM((2, 2, 16, 128), BF),
            pltpu.VMEM((10, 16, 128), BF),
            pltpu.VMEM((10, 16, 128), BF),
            pltpu.VMEM((2, 10, 16, 128), BF),
            pltpu.VMEM((2, 10, 16, 128), BF),
            pltpu.VMEM((320, 384), BF),
            pltpu.VMEM((96, 256), BF),
            pltpu.VMEM((20, 16, 256), F32),
            pltpu.VMEM((20, 64, 256), BF),
            pltpu.VMEM((20, 64, 128), BF),
            pltpu.VMEM((192, 256), BF),
            pltpu.VMEM((3072, 256), BF),
            pltpu.VMEM((2, 256, 128), BF),
            pltpu.VMEM((4608, 256), BF),
            pltpu.VMEM((4608, 256), BF),
            pltpu.VMEM((2, 128, 256), BF),
            pltpu.VMEM((6144, 256), BF),
            pltpu.VMEM((16, 256), F32),
            pltpu.VMEM((18, 368, 256), BF),
            pltpu.VMEM((18, 368, 256), BF),
            pltpu.VMEM((16, 352, 256), BF),
            pltpu.VMEM((3, 8, 176, 256), BF),
            pltpu.VMEM((3, 6, 160, 256), BF),
            pltpu.VMEM((4, 144, 256), BF),
            pltpu.VMEM((2, 2, 6, 128, 256), BF),
            pltpu.VMEM((2, 2, 6, 128, 256), BF),
            pltpu.SemaphoreType.DMA((14,)),
            pltpu.SemaphoreType.DMA((4,)),
            pltpu.SemaphoreType.DMA((4,)),
            pltpu.SemaphoreType.DMA((10,)),
            pltpu.SemaphoreType.DMA((10,)),
            pltpu.SemaphoreType.DMA((2,)),
            pltpu.SemaphoreType.DMA((2,)),
        ],
        compiler_params=pltpu.CompilerParams(
            vmem_limit_bytes=58 * 1024 * 1024, collective_id=0, has_side_effects=True
        ),
    )(*args)
    return d.astype(F32) + jnp.transpose(out, (0, 1, 3, 2))


def solution(mesh):
    placed = (P(None, "gx", "gy", "gz"), P(), P(), P(), P(), P(), P(), P(), P())
    return jax.shard_map(
        local, mesh=mesh, in_specs=placed, out_specs=P(None, "gx", "gy", "gz"), check_vma=False
    )
```
